32 devices in a mesh: sub: 4 (over z), data: 8 (over y, x, core).
Axes of the slice: x: 2, y: 2, z: 4, core: 2. Of those that a mesh axis runs over, the one named last changes fastest.
Arguments:
- x_act: bfloat16 [128, 196, 384], P(('data', 'sub'))
- y_tgt: bfloat16 [128, 196, 384], P(('data', 'sub'))
- w_in: float32 [8, 384, 1536], replicated
- w_out: float32 [8, 1536, 384], replicated
Outputs:
- output 1: float32 [8, 384, 1536], replicated
- output 2: float32 [8, 1536, 384], replicated
- output 3: float32 [], replicated
All inputs are finite; a program needn't handle non-finite values.
Results may differ from the reference program's by a relative error of at most 0.00120099.
Values are sent between devices in bfloat16 or wider.
A program may use at most 1 GiB of HBM per device.

```python
import jax
import jax.numpy as jnp
from jax import lax

MODEL_DIM = 384
MLP_DIM = 1536
SEQ_LEN = 196
LAYERS = 8
IMAGES_DEV = 4
SUB_SIZE = 4
DATA_SIZE = 8
RHO_SCALE = 0.1
STEP_SIZE = 1.0


def setup_inputs(seed: int = 0) -> dict:
    root_key = jax.random.key(seed)
    key_x, key_y, key_in, key_out, key_scale = jax.random.split(root_key, 5)
    batch_size = IMAGES_DEV * SUB_SIZE * DATA_SIZE
    act_shape = (batch_size, SEQ_LEN, MODEL_DIM)
    x_act = jax.random.normal(key_x, act_shape, jnp.float32)
    y_tgt = jax.random.normal(key_y, act_shape, jnp.float32)
    w_in = jax.random.normal(key_in, (LAYERS, MODEL_DIM, MLP_DIM), jnp.float32) * MODEL_DIM ** -0.5
    layer_scale = jax.random.uniform(key_scale, (LAYERS, 1, 1), jnp.float32, 0.5, 1.5)
    w_out = jax.random.normal(key_out, (LAYERS, MLP_DIM, MODEL_DIM), jnp.float32) * layer_scale * (MLP_DIM * LAYERS) ** -0.5
    return {"x_act": x_act.astype(jnp.bfloat16), "y_tgt": y_tgt.astype(jnp.bfloat16), "w_in": w_in, "w_out": w_out}


def gelu_exact(pre_act):
    return jax.nn.gelu(pre_act, approximate=False)


def local_grads(tok_in, tok_tgt, w_in_b, w_out_b):
    def fwd_layer(hid_in, layer_w):
        w_in_l, w_out_l = layer_w
        pre_act = jnp.dot(hid_in, w_in_l, preferred_element_type=jnp.float32).astype(jnp.bfloat16)
        gelu_out = gelu_exact(pre_act.astype(jnp.float32)).astype(jnp.bfloat16)
        branch = jnp.dot(gelu_out, w_out_l, preferred_element_type=jnp.float32)
        hid_next = (hid_in.astype(jnp.float32) + branch).astype(jnp.bfloat16)
        return hid_next, (hid_in, pre_act, gelu_out)
    final_hid, saved_acts = lax.scan(fwd_layer, tok_in, (w_in_b, w_out_b))
    res_diff = final_hid.astype(jnp.float32) - tok_tgt.astype(jnp.float32)
    elem_count = res_diff.size
    loss_val = 0.5 * jnp.sum(res_diff * res_diff) / elem_count
    back_err = (res_diff / elem_count).astype(jnp.bfloat16)

    def bwd_layer(err_in, layer_data):
        w_in_l, w_out_l, hid_in, pre_act, gelu_out = layer_data
        grad_out = jnp.dot(gelu_out.T, err_in, preferred_element_type=jnp.float32).astype(jnp.bfloat16)
        d_act = jnp.dot(err_in, w_out_l.T, preferred_element_type=jnp.float32).astype(jnp.bfloat16)
        gelu_vjp = jax.vjp(gelu_exact, pre_act.astype(jnp.float32))[1]
        d_pre = gelu_vjp(d_act.astype(jnp.float32))[0].astype(jnp.bfloat16)
        grad_in = jnp.dot(hid_in.T, d_pre, preferred_element_type=jnp.float32).astype(jnp.bfloat16)
        err_next = (err_in.astype(jnp.float32) + jnp.dot(d_pre, w_in_l.T, preferred_element_type=jnp.float32)).astype(jnp.bfloat16)
        return err_next, (grad_in, grad_out)
    hid_acts, pre_acts, gelu_outs = saved_acts
    back_res = lax.scan(bwd_layer, back_err, (w_in_b, w_out_b, hid_acts, pre_acts, gelu_outs), reverse=True)
    grad_in, grad_out = back_res[1]
    return loss_val, grad_in, grad_out


def reference(x_act, y_tgt, w_in, w_out):
    tok_rows = IMAGES_DEV * SEQ_LEN
    dev_count = SUB_SIZE * DATA_SIZE
    x_dev = x_act.reshape(DATA_SIZE, SUB_SIZE, tok_rows, MODEL_DIM)
    y_dev = y_tgt.reshape(DATA_SIZE, SUB_SIZE, tok_rows, MODEL_DIM)
    rho_val = RHO_SCALE * MODEL_DIM ** 0.5
    w_in_b = w_in.astype(jnp.bfloat16)
    w_out_b = w_out.astype(jnp.bfloat16)
    zero_in = jnp.zeros(w_in.shape, jnp.float32)
    zero_out = jnp.zeros(w_out.shape, jnp.float32)

    def group_step(carry_sums, group_data):
        x_grp, y_grp = group_data

        def first_dev(acc_sums, dev_data):
            grads = local_grads(dev_data[0], dev_data[1], w_in_b, w_out_b)
            return (acc_sums[0] + grads[1].astype(jnp.float32), acc_sums[1] + grads[2].astype(jnp.float32)), None
        first_res = lax.scan(first_dev, (zero_in, zero_out), (x_grp, y_grp))
        mean_in = first_res[0][0] / SUB_SIZE
        mean_out = first_res[0][1] / SUB_SIZE
        grad_norm = jnp.sqrt(jnp.sum(mean_in * mean_in) + jnp.sum(mean_out * mean_out))
        eps_scale = rho_val / grad_norm
        pert_in = (w_in + eps_scale * mean_in).astype(jnp.bfloat16)
        pert_out = (w_out + eps_scale * mean_out).astype(jnp.bfloat16)

        def second_dev(acc_sums, dev_data):
            loss_val, grad_in, grad_out = local_grads(dev_data[0], dev_data[1], pert_in, pert_out)
            return (acc_sums[0] + grad_in.astype(jnp.float32), acc_sums[1] + grad_out.astype(jnp.float32), acc_sums[2] + loss_val), None
        second_res = lax.scan(second_dev, carry_sums, (x_grp, y_grp))
        return second_res[0], None

    totals = lax.scan(group_step, (zero_in, zero_out, jnp.zeros((), jnp.float32)), (x_dev, y_dev))[0]
    w_in_new = w_in - STEP_SIZE * (totals[0] / dev_count)
    w_out_new = w_out - STEP_SIZE * (totals[1] / dev_count)
    return w_in_new, w_out_new, totals[2] / dev_count
```

```python
import jax, jax.numpy as jnp, functools
from jax import lax
from jax.experimental import pallas as pl
from jax.experimental.pallas import tpu as pltpu
from jax.sharding import PartitionSpec as P

F32, BF16 = jnp.float32, jnp.bfloat16
RHO_SCALE = 0.1
STEP_SIZE = 1.0
L, T, D, F = 8, 784, 384, 1536
FT = 256
NT = F // FT
RC, CC = 112, 128
SQRT_HALF = 0.5 ** 0.5
INV_SQRT_2PI = 0.3989422804014327


def gelu_only(z):
    return z * (0.5 + 0.5 * lax.erf(z * SQRT_HALF))


def gelu_both(z):
    cdf = 0.5 + 0.5 * lax.erf(z * SQRT_HALF)
    pdf = INV_SQRT_2PI * jnp.exp(-0.5 * (z * z))
    return z * cdf, cdf + z * pdf


def chunks(col0):
    for c in range(FT // CC):
        for r in range(T // RC):
            yield slice(r * RC, (r + 1) * RC), slice(col0 + c * CC, col0 + (c + 1) * CC)


def dot(a, b, ca=1, cb=0):
    return lax.dot_general(a, b, (((ca,), (cb,)), ((), ())), preferred_element_type=F32)


def pass_kernel(x_ref, y_ref, vin_ref, vout_ref, gin_ref, gout_ref, loss_ref, h_s, z_s, a_s, q_s, e_s, hT_s):
    step = pl.program_id(0)

    @pl.when(step == 0)
    def _():
        h_s[0] = x_ref[...]

    @pl.when(step < L)
    def _():
        lay = step
        z_l = z_s.at[lay]
        h = h_s[lay]
        for j in range(NT):
            cols = slice(j * FT, (j + 1) * FT)
            z_l[:, cols] = dot(h, vin_ref[0, :, cols]).astype(BF16)
            for rs, cs in chunks(j * FT):
                a_s[rs, cs] = gelu_only(z_l[rs, cs].astype(F32)).astype(BF16)
        out = (h.astype(F32) + dot(a_s[...], vout_ref[0])).astype(BF16)
        h_s[lay + 1] = out

    @pl.when(step == L - 1)
    def _():
        diff = h_s[L].astype(F32) - y_ref[...].astype(F32)
        loss_ref[0, 0] = 0.5 * jnp.sum(diff * diff) / (T * D)
        e_s[...] = (diff / (T * D)).astype(BF16)

    @pl.when(step >= L)
    def _():
        lay = 2 * L - 1 - step
        z_l = z_s.at[lay]
        e = e_s[...]
        hT_s[...] = h_s[lay].T
        for j in range(NT):
            cols = slice(j * FT, (j + 1) * FT)
            q_s[:, cols] = dot(e, vout_ref[0, cols, :], 1, 1).astype(BF16)
            for rs, cs in chunks(j * FT):
                act, slope = gelu_both(z_l[rs, cs].astype(F32))
                a_s[rs, cs] = act.astype(BF16)
                q_s[rs, cs] = (slope * q_s[rs, cs].astype(F32)).astype(BF16)
            gout_ref[0, cols, :] = dot(a_s[:, cols], e, 0, 0).astype(BF16)
            gin_ref[0, :, cols] = dot(hT_s[...], q_s[:, cols]).astype(BF16)
        e_s[...] = (e.astype(F32) + dot(q_s[...], vin_ref[0], 1, 1)).astype(BF16)


def run_pass(x, y, vin, vout):
    lay = lambda s: jnp.where(s < L, s, 2 * L - 1 - s)
    glay = lambda s: jnp.where(s < L, L - 1, 2 * L - 1 - s)
    return pl.pallas_call(
        pass_kernel,
        grid=(2 * L,),
        in_specs=[
            pl.BlockSpec((T, D), lambda s: (0, 0)),
            pl.BlockSpec((T, D), lambda s: (0, 0)),
            pl.BlockSpec((1, D, F), lambda s: (lay(s), 0, 0)),
            pl.BlockSpec((1, F, D), lambda s: (lay(s), 0, 0)),
        ],
        out_specs=[
            pl.BlockSpec((1, D, F), lambda s: (glay(s), 0, 0)),
            pl.BlockSpec((1, F, D), lambda s: (glay(s), 0, 0)),
            pl.BlockSpec(memory_space=pltpu.SMEM),
        ],
        out_shape=[
            jax.ShapeDtypeStruct((L, D, F), BF16),
            jax.ShapeDtypeStruct((L, F, D), BF16),
            jax.ShapeDtypeStruct((1, 1), F32),
        ],
        scratch_shapes=[
            pltpu.VMEM((L + 1, T, D), BF16),
            pltpu.VMEM((L, T, F), BF16),
            pltpu.VMEM((T, F), BF16),
            pltpu.VMEM((T, F), BF16),
            pltpu.VMEM((T, D), BF16),
            pltpu.VMEM((D, T), BF16),
        ],
        compiler_params=pltpu.CompilerParams(vmem_limit_bytes=60 * 2**20),
        cost_estimate=pl.CostEstimate(flops=L * 12 * T * D * F, bytes_accessed=4 * L * D * F * 2, transcendentals=0),
    )(x, y, vin, vout)


def move_pairs(sub_size, data_size, flip):
    pairs = []
    for shard in range(sub_size):
        for data_idx in range(data_size):
            group = data_idx % 2
            chip = 2 * group + ((shard + flip) % 2)
            pairs.append((shard * data_size + data_idx, chip * data_size + data_idx - group + shard // 2))
    return pairs


def solution(mesh):
    sub_size, data_size = mesh.shape["sub"], mesh.shape["data"]
    dev_count = sub_size * data_size
    axes = ("sub", "data")
    core_swap = [(i, i ^ 1) for i in range(data_size)]

    def swap(v):
        return lax.ppermute(v, "data", core_swap)

    def device_step(x_blk, y_blk, w_in, w_out):
        tok = jnp.stack([x_blk.reshape(T, D), y_blk.reshape(T, D)])
        own = lax.ppermute(tok, axes, move_pairs(sub_size, data_size, 0))
        other = lax.ppermute(tok, axes, move_pairs(sub_size, data_size, 1))
        v_in, v_out = w_in.astype(BF16), w_out.astype(BF16)
        a_in, a_out, _ = run_pass(own[0], own[1], v_in, v_out)
        pa_in, pa_out = swap(a_in), swap(a_out)
        b_in, b_out, _ = run_pass(other[0], other[1], v_in, v_out)
        pb_in, pb_out = swap(b_in), swap(b_out)
        f = lambda v: v.astype(F32)
        mean_in = ((f(a_in) + f(b_in)) + (f(pa_in) + f(pb_in))) / sub_size
        mean_out = ((f(a_out) + f(b_out)) + (f(pa_out) + f(pb_out))) / sub_size
        grad_norm = jnp.sqrt(jnp.sum(mean_in * mean_in) + jnp.sum(mean_out * mean_out))
        scale = RHO_SCALE * D ** 0.5 / grad_norm
        t_in = (w_in + scale * mean_in).astype(BF16)
        t_out = (w_out + scale * mean_out).astype(BF16)
        n_in, n_out, loss = run_pass(own[0], own[1], t_in, t_out)
        idx = lax.axis_index(axes)

        def update(w, g):
            flat = f(g).reshape(-1, g.shape[-1])
            part = lax.psum_scatter(flat, axes, scatter_dimension=0, tiled=True)
            rows = part.shape[0]
            w_part = lax.dynamic_slice_in_dim(w.reshape(flat.shape), idx * rows, rows, 0)
            new = w_part - STEP_SIZE * (part / dev_count)
            return lax.all_gather(new, axes, axis=0, tiled=True).reshape(w.shape)

        return update(w_in, n_in), update(w_out, n_out), lax.psum(loss[0, 0], axes) / dev_count

    batch_spec = P(("data", "sub"))
    return jax.shard_map(device_step, mesh=mesh, in_specs=(batch_spec, batch_spec, P(), P()), out_specs=(P(), P(), P()), check_vma=False)
```

```python
import jax, jax.numpy as jnp, functools
from jax import lax
from jax.experimental import pallas as pl
from jax.experimental.pallas import tpu as pltpu
from jax.sharding import PartitionSpec as P

F32, BF16 = jnp.float32, jnp.bfloat16
RHO_SCALE = 0.1
STEP_SIZE = 1.0
L, T, D, F = 8, 784, 384, 1536
FT = 256
NT = F // FT
RC, CC = 112, 128
SQRT_HALF = 0.5 ** 0.5
INV_SQRT_2PI = 0.3989422804014327


def gelu_only(z):
    return z * (0.5 + 0.5 * lax.erf(z * SQRT_HALF))


def gelu_both(z):
    cdf = 0.5 + 0.5 * lax.erf(z * SQRT_HALF)
    pdf = INV_SQRT_2PI * jnp.exp(-0.5 * (z * z))
    return z * cdf, cdf + z * pdf


def chunks(col0):
    for c in range(FT // CC):
        for r in range(T // RC):
            yield slice(r * RC, (r + 1) * RC), slice(col0 + c * CC, col0 + (c + 1) * CC)


def dot(a, b, ca=1, cb=0):
    return lax.dot_general(a, b, (((ca,), (cb,)), ((), ())), preferred_element_type=F32)


def pass_kernel(x_ref, y_ref, vin_ref, vout_ref, gin_ref, gout_ref, loss_ref, h_s, z_s, a_s, q_s, e_s, hT_s):
    step = pl.program_id(0)

    @pl.when(step == 0)
    def _():
        h_s[0] = x_ref[...]

    @pl.when(step < L)
    def _():
        lay = step
        z_l = z_s.at[lay]
        h = h_s[lay]
        for j in range(NT):
            cols = slice(j * FT, (j + 1) * FT)
            z_l[:, cols] = dot(h, vin_ref[0, :, cols]).astype(BF16)
            for rs, cs in chunks(j * FT):
                a_s[rs, cs] = gelu_only(z_l[rs, cs].astype(F32)).astype(BF16)
        out = (h.astype(F32) + dot(a_s[...], vout_ref[0])).astype(BF16)
        h_s[lay + 1] = out

    @pl.when(step == L - 1)
    def _():
        diff = h_s[L].astype(F32) - y_ref[...].astype(F32)
        loss_ref[0, 0] = 0.5 * jnp.sum(diff * diff) / (T * D)
        e_s[...] = (diff / (T * D)).astype(BF16)

    @pl.when(step >= L)
    def _():
        lay = 2 * L - 1 - step
        z_l = z_s.at[lay]
        e = e_s[...]
        hT_s[...] = h_s[lay].T
        for j in range(NT):
            cols = slice(j * FT, (j + 1) * FT)
            q_s[:, cols] = dot(e, vout_ref[0, cols, :], 1, 1).astype(BF16)
            for rs, cs in chunks(j * FT):
                act, slope = gelu_both(z_l[rs, cs].astype(F32))
                a_s[rs, cs] = act.astype(BF16)
                q_s[rs, cs] = (slope * q_s[rs, cs].astype(F32)).astype(BF16)
            gout_ref[0, cols, :] = dot(a_s[:, cols], e, 0, 0).astype(BF16)
            gin_ref[0, :, cols] = dot(hT_s[...], q_s[:, cols]).astype(BF16)
        e_s[...] = (e.astype(F32) + dot(q_s[...], vin_ref[0], 1, 1)).astype(BF16)


def run_pass(x, y, vin, vout):
    lay = lambda s: jnp.where(s < L, s, 2 * L - 1 - s)
    glay = lambda s: jnp.where(s < L, L - 1, 2 * L - 1 - s)
    return pl.pallas_call(
        pass_kernel,
        grid=(2 * L,),
        in_specs=[
            pl.BlockSpec((T, D), lambda s: (0, 0)),
            pl.BlockSpec((T, D), lambda s: (0, 0)),
            pl.BlockSpec((1, D, F), lambda s: (lay(s), 0, 0)),
            pl.BlockSpec((1, F, D), lambda s: (lay(s), 0, 0)),
        ],
        out_specs=[
            pl.BlockSpec((1, D, F), lambda s: (glay(s), 0, 0)),
            pl.BlockSpec((1, F, D), lambda s: (glay(s), 0, 0)),
            pl.BlockSpec(memory_space=pltpu.SMEM),
        ],
        out_shape=[
            jax.ShapeDtypeStruct((L, D, F), BF16),
            jax.ShapeDtypeStruct((L, F, D), BF16),
            jax.ShapeDtypeStruct((1, 1), F32),
        ],
        scratch_shapes=[
            pltpu.VMEM((L + 1, T, D), BF16),
            pltpu.VMEM((L, T, F), BF16),
            pltpu.VMEM((T, F), BF16),
            pltpu.VMEM((T, F), BF16),
            pltpu.VMEM((T, D), BF16),
            pltpu.VMEM((D, T), BF16),
        ],
        compiler_params=pltpu.CompilerParams(vmem_limit_bytes=60 * 2**20),
        cost_estimate=pl.CostEstimate(flops=L * 12 * T * D * F, bytes_accessed=4 * L * D * F * 2, transcendentals=0),
    )(x, y, vin, vout)


ROWS = (384, 768)
COLS = (768, 384)
STAGES = 7
MESH_ID = pl.DeviceIdType.MESH


def al(v, n):
    return pl.multiple_of(v, n)


def half_at(ref, kind, lay, core, row, rows):
    if kind == 0:
        return ref.at[lay, pl.ds(al(row, 8), rows), pl.ds(al(core * COLS[0], 128), COLS[0])]
    return ref.at[lay, pl.ds(al(core * ROWS[1] + row, 8), rows), :]


def row_loop(rows, block, body):
    def step(i, _):
        body(al(i * block, block))
        return 0
    lax.fori_loop(0, rows // block, step, 0)


class Place:
    def __init__(self):
        z, data = lax.axis_index("sub"), lax.axis_index("data")
        core, xx, yy = lax.rem(data, 2), lax.rem(data // 2, 2), data // 4
        self.core, self.z = core, z
        flips = (2 - 4 * xx, 4 - 8 * yy)
        self.partner = (z, data + 1 - 2 * core)
        self.first = tuple((z, data + f) for f in flips)
        self.second = (self.first[1], self.first[0])
        self.c1, self.c2 = (xx, yy), (yy, xx)
        self.zs = [lax.rem(z + d, 4) for d in (1, 2, 3)]
        self.z_peers = [(zt, data) for zt in self.zs]

    def barrier(self, peers):
        sem = pltpu.get_barrier_semaphore()
        for peer in peers:
            pl.semaphore_signal(sem, inc=1, device_id=peer, device_id_type=MESH_ID)
        pl.semaphore_wait(sem, len(peers))


def remote(src, dst, send, recv, peer):
    return pltpu.make_async_remote_copy(src_ref=src, dst_ref=dst, send_sem=send, recv_sem=recv, device_id=peer, device_id_type=MESH_ID)


def exch_kernel(count, g0, g1, w0, w1, loss_ref, o0, o1, lout,
                own0, own1, d0, d1, r10, r11, r20, r21, r30, r31, s10, s11, s20, s21, s30, s31, nb0, nb1, wb0, wb1, lt, lr,
                own_sem, w_sem, d_sem, r1_sem, r2_sem, r3_sem, az_sem, a2_sem, a1_sem, ad_sem,
                ds_sem, s1_sem, s2_sem, s3_sem, zs_sem, n_sem, a2s_sem, a1s_sem, ads_sem, l_sem, ls_sem):
    me = Place()
    core, z = me.core, me.z
    g, w, o = (g0, g1), (w0, w1), (o0, o1)
    own, dd, r1, r2, r3 = (own0, own1), (d0, d1), (r10, r11), (r20, r21), (r30, r31)
    s1, s2, s3, nb, wb = (s10, s11), (s20, s21), (s30, s31), (nb0, nb1), (wb0, wb1)
    kinds = (0, 1)
    me.barrier([me.partner, me.first[0], me.first[1]] + me.z_peers)

    def quarter(kind):
        return (2 * me.c1[kind] + me.c2[kind]) * (ROWS[kind] // 4)

    def own_copy(l, k):
        return pltpu.make_async_copy(half_at(g[k], k, l, core, 0, ROWS[k]), own[k].at[l], own_sem.at[l, k])

    def w_copy(l, k):
        n = ROWS[k] // 16
        return pltpu.make_async_copy(half_at(w[k], k, l, core, quarter(k) + z * n, n), wb[k].at[l], w_sem.at[l, k])

    def d_copy(l, k):
        return remote(half_at(g[k], k, l, 1 - core, 0, ROWS[k]), dd[k].at[l], ds_sem.at[l, k], d_sem.at[l, k], me.partner)

    def r1_copy(l, k):
        slot = lax.rem(l, 2)
        return remote(s1[k].at[slot], r1[k].at[l], s1_sem.at[slot, k], r1_sem.at[l, k], me.first[k])

    def r2_copy(l, k):
        slot = lax.rem(l, 2)
        return remote(s2[k].at[slot], r2[k].at[l], s2_sem.at[slot, k], r2_sem.at[l, k], me.second[k])

    def r3_copy(l, k, j):
        slot, n = lax.rem(l, 2), ROWS[k] // 16
        return remote(s3[k].at[slot, pl.ds(al(me.zs[j] * n, 8), n)], r3[k].at[l, 2 - j], s3_sem.at[slot, k, j], r3_sem.at[l, k, 2 - j], me.z_peers[j])

    def piece(l, k, zi):
        n = ROWS[k] // 16
        return half_at(o[k], k, l, core, quarter(k) + zi * n, n)

    def az_copy(l, k, j):
        slot = lax.rem(l, 2)
        return remote(nb[k].at[slot], piece(l, k, z), zs_sem.at[slot, k, j], az_sem.at[l, k, 2 - j], me.z_peers[j])

    def n_copy(l, k):
        slot = lax.rem(l, 2)
        return pltpu.make_async_copy(nb[k].at[slot], piece(l, k, z), n_sem.at[slot, k])

    def gather(l, k, row, rows, send, recv, peer):
        part = half_at(o[k], k, l, core, row, rows)
        return remote(part, part, send.at[lax.rem(l, 2), k], recv.at[l, k], peer)

    def a2_copy(l, k):
        return gather(l, k, quarter(k), ROWS[k] // 4, a2s_sem, a2_sem, me.second[k])

    def a1_copy(l, k):
        return gather(l, k, me.c1[k] * (ROWS[k] // 2), ROWS[k] // 2, a1s_sem, a1_sem, me.first[k])

    def ad_copy(l, k):
        return gather(l, k, 0, ROWS[k], ads_sem, ad_sem, me.partner)

    def both(k, l, row, n):
        return own[k][l, pl.ds(row, n), :].astype(F32) + dd[k][l, pl.ds(row, n), :].astype(F32)

    def start(l, k):
        d_copy(l, k).start()
        own_copy(l, k).start()
        w_copy(l, k).start()

    def stage0(l, k):
        own_copy(l, k).wait()
        d_copy(l, k).wait_recv()

        @pl.when(l >= 2)
        def _():
            r1_copy(l - 2, k).wait_send()
        n, slot = ROWS[k] // 2, lax.rem(l, 2)
        base = (1 - me.c1[k]) * n

        def body(row):
            s1[k][slot, pl.ds(row, 16), :] = both(k, l, al(base + row, 16), 16)
        row_loop(n, 16, body)
        r1_copy(l, k).start()

    def stage1(l, k):
        r1_copy(l, k).wait_recv()

        @pl.when(l >= 2)
        def _():
            r2_copy(l - 2, k).wait_send()
        n, slot = ROWS[k] // 4, lax.rem(l, 2)
        in_half = (1 - me.c2[k]) * n
        base = me.c1[k] * 2 * n + in_half

        def body(row):
            s2[k][slot, pl.ds(row, 16), :] = both(k, l, al(base + row, 16), 16) + r1[k][l, pl.ds(al(in_half + row, 16), 16), :]
        row_loop(n, 16, body)
        r2_copy(l, k).start()

    def stage2(l, k):
        r2_copy(l, k).wait_recv()

        @pl.when(l >= 2)
        def _():
            for j in range(3):
                r3_copy(l - 2, k, j).wait_send()
        n, slot = ROWS[k] // 4, lax.rem(l, 2)
        in_half = me.c2[k] * n
        base = me.c1[k] * 2 * n + in_half

        def body(row):
            s3[k][slot, pl.ds(row, 16), :] = (both(k, l, al(base + row, 16), 16) + r1[k][l, pl.ds(al(in_half + row, 16), 16), :]) + r2[k][l, pl.ds(row, 16), :]
        row_loop(n, 16, body)
        for j in range(3):
            r3_copy(l, k, j).start()

    def stage3(l, k):
        for j in range(3):
            r3_copy(l, k, j).wait_recv()
        w_copy(l, k).wait()

        @pl.when(l >= 2)
        def _():
            for j in range(3):
                az_copy(l - 2, k, j).wait_send()
        n, slot = ROWS[k] // 16, lax.rem(l, 2)

        def body(row):
            rs = pl.ds(row, 8)
            tot = (s3[k][slot, pl.ds(al(z * n + row, 8), 8), :] + r3[k][l, 0, rs, :]) + (r3[k][l, 1, rs, :] + r3[k][l, 2, rs, :])
            nb[k][slot, rs, :] = wb[k][l, rs, :] - STEP_SIZE * (tot * (1.0 / count))
        row_loop(n, 8, body)
        n_copy(l, k).start()
        for j in range(3):
            az_copy(l, k, j).start()

    def stage4(l, k):
        n_copy(l, k).wait()
        for j in range(3):
            az_copy(l, k, j).wait_recv()

        @pl.when(l >= 2)
        def _():
            a2_copy(l - 2, k).wait_send()
        a2_copy(l, k).start()

    def stage5(l, k):
        a2_copy(l, k).wait_recv()

        @pl.when(l >= 2)
        def _():
            a1_copy(l - 2, k).wait_send()
        a1_copy(l, k).start()

    def stage6(l, k):
        a1_copy(l, k).wait_recv()

        @pl.when(l >= 2)
        def _():
            ad_copy(l - 2, k).wait_send()
        ad_copy(l, k).start()

    stages = (stage0, stage1, stage2, stage3, stage4, stage5, stage6)

    def loss_copy(i, peer, j):
        return remote(lt.at[i], lr.at[j], ls_sem.at[j], l_sem.at[j], peer)

    loss_hops = [[(me.partner, 0)], [(me.first[0], 1)], [(me.first[1], 2)], [(me.z_peers[j], 3 + j) for j in range(3)]]

    def loss_wait(i):
        for peer, j in loss_hops[i]:
            loss_copy(i, peer, j).wait()
        tot = lt[i]
        for _, j in loss_hops[i]:
            tot = tot + (lr[j] if i < 3 else lr[8 - j])
        return tot

    lt[0] = jnp.full((8, 128), loss_ref[0, 0], F32)

    def start_all(l, _):
        for k in kinds:
            start(l, k)
        return 0
    lax.fori_loop(0, L, start_all, 0)

    def loss_step(t):
        for i in range(5):
            @pl.when(t == i)
            def _(i=i):
                if i > 0:
                    tot = loss_wait(i - 1)
                    if i == 4:
                        lout[...] = tot * (1.0 / count)
                    else:
                        lt[i] = tot
                if i < 4:
                    for peer, j in loss_hops[i]:
                        loss_copy(i, peer, j).start()

    def tick(t, _):
        loss_step(t)
        for s in reversed(range(STAGES)):
            l = t - s

            @pl.when(jnp.logical_and(l >= 0, l < L))
            def _(s=s, l=l):
                for k in kinds:
                    stages[s](l, k)
        return 0
    lax.fori_loop(0, L + STAGES - 1, tick, 0)

    def finish(l, _):
        for k in kinds:
            ad_copy(l, k).wait_recv()
            d_copy(l, k).wait_send()
        return 0
    lax.fori_loop(0, L, finish, 0)
    for l in (L - 2, L - 1):
        for k in kinds:
            r1_copy(l, k).wait_send()
            r2_copy(l, k).wait_send()
            for j in range(3):
                r3_copy(l, k, j).wait_send()
                az_copy(l, k, j).wait_send()
            a2_copy(l, k).wait_send()
            a1_copy(l, k).wait_send()
            ad_copy(l, k).wait_send()


def exchange(count, g_in, g_out, w_in, w_out, loss):
    def per_kind(lead, div, dtype):
        return [pltpu.VMEM(lead + (ROWS[k] // div, COLS[k]), dtype) for k in (0, 1)]
    dma = pltpu.SemaphoreType.DMA
    any_spec = pl.BlockSpec(memory_space=pl.ANY)
    scratch = (per_kind((L,), 1, BF16) + per_kind((L,), 1, BF16) + per_kind((L,), 2, F32) + per_kind((L,), 4, F32)
               + per_kind((L, 3), 16, F32) + per_kind((2,), 2, F32) + per_kind((2,), 4, F32) + per_kind((2,), 4, F32)
               + per_kind((2,), 16, F32) + per_kind((L,), 16, F32) + [pltpu.VMEM((4, 8, 128), F32), pltpu.VMEM((6, 8, 128), F32)]
               + [dma((L, 2))] * 5 + [dma((L, 2, 3))] * 2 + [dma((L, 2))] * 4
               + [dma((2, 2))] * 2 + [dma((2, 2, 3))] * 2 + [dma((2, 2))] * 4 + [dma((6,))] * 2)
    return pl.pallas_call(
        functools.partial(exch_kernel, count),
        in_specs=[any_spec] * 4 + [pl.BlockSpec(memory_space=pltpu.SMEM)],
        out_specs=[any_spec, any_spec, pl.BlockSpec(memory_space=pltpu.VMEM)],
        out_shape=[jax.ShapeDtypeStruct((L, D, F), F32), jax.ShapeDtypeStruct((L, F, D), F32), jax.ShapeDtypeStruct((8, 128), F32)],
        scratch_shapes=scratch,
        compiler_params=pltpu.CompilerParams(collective_id=1, has_side_effects=True, vmem_limit_bytes=60 * 2**20),
    )(g_in, g_out, w_in, w_out, loss)


def ascent_kernel(group, a0, a1, b0, b1, w0, w1, t0, t1, oa0, oa1, ob0, ob1, pa0, pa1, pb0, pb1, wb0, wb1, tb0, tb1, nt,
                  o_sem, p_sem, ps_sem, w_sem, tl_sem, ts_sem, tr_sem, n_sem):
    me = Place()
    core = me.core
    src, w, t = ((a0, a1), (b0, b1)), (w0, w1), (t0, t1)
    own, peer = ((oa0, oa1), (ob0, ob1)), ((pa0, pa1), (pb0, pb1))
    wb, tb, kinds = (wb0, wb1), (tb0, tb1), (0, 1)
    me.barrier([me.partner])

    def own_copy(l, k, i):
        return pltpu.make_async_copy(half_at(src[i][k], k, l, core, 0, ROWS[k]), own[i][k].at[l], o_sem.at[l, k, i])

    def peer_copy(l, k, i):
        return remote(half_at(src[i][k], k, l, 1 - core, 0, ROWS[k]), peer[i][k].at[l], ps_sem.at[l, k, i], p_sem.at[l, k, i], me.partner)

    def w_copy(l, k):
        slot = lax.rem(l, 2)
        return pltpu.make_async_copy(half_at(w[k], k, l, core, 0, ROWS[k]), wb[k].at[slot], w_sem.at[slot, k])

    def t_half(l, k):
        return half_at(t[k], k, l, core, 0, ROWS[k])

    def t_local(l, k):
        slot = lax.rem(l, 2)
        return pltpu.make_async_copy(tb[k].at[slot], t_half(l, k), tl_sem.at[slot, k])

    def t_send(l, k):
        slot = lax.rem(l, 2)
        return remote(tb[k].at[slot], t_half(l, k), ts_sem.at[slot, k], tr_sem.at[l, k], me.partner)

    def mean_rows(l, k, row):
        rs = pl.ds(row, 16)
        f = lambda ref: ref[l, rs, :].astype(F32)
        return ((f(own[0][k]) + f(own[1][k])) + (f(peer[0][k]) + f(peer[1][k]))) * (1.0 / group)

    def start_all(l, _):
        for k in kinds:
            for i in range(2):
                peer_copy(l, k, i).start()
                own_copy(l, k, i).start()
        return 0
    lax.fori_loop(0, L, start_all, 0)
    for l in range(2):
        for k in kinds:
            w_copy(l, k).start()

    def square_layer(l, acc):
        for k in kinds:
            for i in range(2):
                own_copy(l, k, i).wait()
                peer_copy(l, k, i).wait_recv()

            def body(i, tot, k=k):
                g = mean_rows(l, k, al(i * 16, 16))
                sq = g * g
                parts = [sq[r:r + 8, c:c + 128] for r in (0, 8) for c in range(0, COLS[k], 128)]
                while len(parts) > 1:
                    parts = [u + v for u, v in zip(parts[::2], parts[1::2])] + parts[len(parts) & ~1:]
                return tot + parts[0]
            acc = lax.fori_loop(0, ROWS[k] // 16, body, acc)
        return acc
    nt[0] = lax.fori_loop(0, L, square_layer, jnp.zeros((8, 128), F32))
    norm_copy = remote(nt.at[0], nt.at[1], n_sem.at[0], n_sem.at[1], me.partner)
    norm_copy.start()
    norm_copy.wait()
    total = jnp.sum(jnp.sum(nt[0] + nt[1], axis=0, keepdims=True), axis=1, keepdims=True)
    scale = (RHO_SCALE * D ** 0.5) / jnp.sqrt(total)

    def move_layer(l, _):
        for k in kinds:
            slot = lax.rem(l, 2)
            w_copy(l, k).wait()

            @pl.when(l >= 2)
            def _(k=k):
                t_local(l - 2, k).wait()
                t_send(l - 2, k).wait_send()

            def body(row, k=k, slot=slot):
                rs = pl.ds(row, 16)
                tb[k][slot, rs, :] = (wb[k][slot, rs, :] + scale * mean_rows(l, k, row)).astype(BF16)
            row_loop(ROWS[k], 16, body)
            t_send(l, k).start()
            t_local(l, k).start()

            @pl.when(l < L - 2)
            def _(k=k):
                w_copy(l + 2, k).start()
        return 0
    lax.fori_loop(0, L, move_layer, 0)

    def finish(l, _):
        for k in kinds:
            t_send(l, k).wait_recv()
            for i in range(2):
                peer_copy(l, k, i).wait_send()
        return 0
    lax.fori_loop(0, L, finish, 0)
    for l in (L - 2, L - 1):
        for k in kinds:
            t_local(l, k).wait()
            t_send(l, k).wait_send()


def ascent(group, first, second, w_in, w_out):
    def per_kind(lead, dtype):
        return [pltpu.VMEM((lead, ROWS[k], COLS[k]), dtype) for k in (0, 1)]
    dma = pltpu.SemaphoreType.DMA
    any_spec = pl.BlockSpec(memory_space=pl.ANY)
    scratch = (per_kind(L, BF16) * 4 + per_kind(2, F32) + per_kind(2, BF16) + [pltpu.VMEM((2, 8, 128), F32)]
               + [dma((L, 2, 2))] * 3 + [dma((2, 2))] * 3 + [dma((L, 2)), dma((2,))])
    return pl.pallas_call(
        functools.partial(ascent_kernel, group),
        in_specs=[any_spec] * 6,
        out_specs=[any_spec] * 2,
        out_shape=[jax.ShapeDtypeStruct((L, D, F), BF16), jax.ShapeDtypeStruct((L, F, D), BF16)],
        scratch_shapes=scratch,
        compiler_params=pltpu.CompilerParams(collective_id=2, has_side_effects=True, vmem_limit_bytes=60 * 2**20),
    )(*first, *second, w_in, w_out)


def move_pairs(sub_size, data_size, flip):
    pairs = []
    for shard in range(sub_size):
        for data_idx in range(data_size):
            group = data_idx % 2
            chip = 2 * group + ((shard + flip) % 2)
            pairs.append((shard * data_size + data_idx, chip * data_size + data_idx - group + shard // 2))
    return pairs


def solution(mesh):
    sub_size, data_size = mesh.shape["sub"], mesh.shape["data"]
    dev_count = sub_size * data_size
    axes = ("sub", "data")

    def device_step(x_blk, y_blk, w_in, w_out):
        tok = jnp.stack([x_blk.reshape(T, D), y_blk.reshape(T, D)])
        own = lax.ppermute(tok, axes, move_pairs(sub_size, data_size, 0))
        other = lax.ppermute(tok, axes, move_pairs(sub_size, data_size, 1))
        v_in, v_out = w_in.astype(BF16), w_out.astype(BF16)
        first = run_pass(own[0], own[1], v_in, v_out)[:2]
        second = run_pass(other[0], other[1], v_in, v_out)[:2]
        t_in, t_out = ascent(sub_size, first, second, w_in, w_out)
        n_in, n_out, loss = run_pass(own[0], own[1], t_in, t_out)
        new_in, new_out, loss_all = exchange(dev_count, n_in, n_out, w_in, w_out, loss)
        return new_in, new_out, loss_all[0, 0]

    batch_spec = P(("data", "sub"))
    return jax.shard_map(device_step, mesh=mesh, in_specs=(batch_spec, batch_spec, P(), P()), out_specs=(P(), P(), P()), check_vma=False)
```

```python
import jax, jax.numpy as jnp, functools
from jax import lax
from jax.experimental import pallas as pl
from jax.experimental.pallas import tpu as pltpu
from jax.sharding import PartitionSpec as P

F32, BF16 = jnp.float32, jnp.bfloat16
RHO_SCALE = 0.1
STEP_SIZE = 1.0
L, T, D, F = 8, 784, 384, 1536
FT = 256
NT = F // FT
RC, CC = 112, 128
SQRT_HALF = 0.5 ** 0.5
INV_SQRT_2PI = 0.3989422804014327


def gelu_only(z):
    return z * (0.5 + 0.5 * lax.erf(z * SQRT_HALF))


def gelu_both(z):
    cdf = 0.5 + 0.5 * lax.erf(z * SQRT_HALF)
    pdf = INV_SQRT_2PI * jnp.exp(-0.5 * (z * z))
    return z * cdf, cdf + z * pdf


def chunks(col0):
    for c in range(FT // CC):
        for r in range(T // RC):
            yield slice(r * RC, (r + 1) * RC), slice(col0 + c * CC, col0 + (c + 1) * CC)


def dot(a, b, ca=1, cb=0):
    return lax.dot_general(a, b, (((ca,), (cb,)), ((), ())), preferred_element_type=F32)


def pass_kernel(x_ref, y_ref, vin_ref, vout_ref, gin_ref, gout_ref, loss_ref, h_s, z_s, a_s, q_s, e_s, hT_s):
    step = pl.program_id(0)

    @pl.when(step == 0)
    def _():
        h_s[0] = x_ref[...]

    @pl.when(step < L)
    def _():
        lay = step
        z_l = z_s.at[lay]
        h = h_s[lay]
        for j in range(NT):
            cols = slice(j * FT, (j + 1) * FT)
            z_l[:, cols] = dot(h, vin_ref[0, :, cols]).astype(BF16)
            for rs, cs in chunks(j * FT):
                a_s[rs, cs] = gelu_only(z_l[rs, cs].astype(F32)).astype(BF16)
        out = (h.astype(F32) + dot(a_s[...], vout_ref[0])).astype(BF16)
        h_s[lay + 1] = out

    @pl.when(step == L - 1)
    def _():
        diff = h_s[L].astype(F32) - y_ref[...].astype(F32)
        loss_ref[0, 0] = 0.5 * jnp.sum(diff * diff) / (T * D)
        e_s[...] = (diff / (T * D)).astype(BF16)

    @pl.when(step >= L)
    def _():
        lay = 2 * L - 1 - step
        z_l = z_s.at[lay]
        e = e_s[...]
        hT_s[...] = h_s[lay].T
        for j in range(NT):
            cols = slice(j * FT, (j + 1) * FT)
            q_s[:, cols] = dot(e, vout_ref[0, cols, :], 1, 1).astype(BF16)
            for rs, cs in chunks(j * FT):
                act, slope = gelu_both(z_l[rs, cs].astype(F32))
                a_s[rs, cs] = act.astype(BF16)
                q_s[rs, cs] = (slope * q_s[rs, cs].astype(F32)).astype(BF16)
            gout_ref[0, cols, :] = dot(a_s[:, cols], e, 0, 0).astype(BF16)
            gin_ref[0, :, cols] = dot(hT_s[...], q_s[:, cols]).astype(BF16)
        e_s[...] = (e.astype(F32) + dot(q_s[...], vin_ref[0], 1, 1)).astype(BF16)


def run_pass(x, y, vin, vout):
    lay = lambda s: jnp.where(s < L, s, 2 * L - 1 - s)
    glay = lambda s: jnp.where(s < L, L - 1, 2 * L - 1 - s)
    return pl.pallas_call(
        pass_kernel,
        grid=(2 * L,),
        in_specs=[
            pl.BlockSpec((T, D), lambda s: (0, 0)),
            pl.BlockSpec((T, D), lambda s: (0, 0)),
            pl.BlockSpec((1, D, F), lambda s: (lay(s), 0, 0)),
            pl.BlockSpec((1, F, D), lambda s: (lay(s), 0, 0)),
        ],
        out_specs=[
            pl.BlockSpec((1, D, F), lambda s: (glay(s), 0, 0)),
            pl.BlockSpec((1, F, D), lambda s: (glay(s), 0, 0)),
            pl.BlockSpec(memory_space=pltpu.SMEM),
        ],
        out_shape=[
            jax.ShapeDtypeStruct((L, D, F), BF16),
            jax.ShapeDtypeStruct((L, F, D), BF16),
            jax.ShapeDtypeStruct((1, 1), F32),
        ],
        scratch_shapes=[
            pltpu.VMEM((L + 1, T, D), BF16),
            pltpu.VMEM((L, T, F), BF16),
            pltpu.VMEM((T, F), BF16),
            pltpu.VMEM((T, F), BF16),
            pltpu.VMEM((T, D), BF16),
            pltpu.VMEM((D, T), BF16),
        ],
        compiler_params=pltpu.CompilerParams(vmem_limit_bytes=60 * 2**20),
        cost_estimate=pl.CostEstimate(flops=L * 12 * T * D * F, bytes_accessed=4 * L * D * F * 2, transcendentals=0),
    )(x, y, vin, vout)


ROWS = (384, 768)
COLS = (768, 384)
STAGES = 7
MESH_ID = pl.DeviceIdType.MESH


def al(v, n):
    return pl.multiple_of(v, n)


def half_at(ref, kind, lay, core, row, rows):
    if kind == 0:
        return ref.at[lay, pl.ds(al(row, 8), rows), pl.ds(al(core * COLS[0], 128), COLS[0])]
    return ref.at[lay, pl.ds(al(core * ROWS[1] + row, 8), rows), :]


def row_loop(rows, block, body):
    def step(i, _):
        body(al(i * block, block))
        return 0
    lax.fori_loop(0, rows // block, step, 0)


class Place:
    def __init__(self):
        z, data = lax.axis_index("sub"), lax.axis_index("data")
        core, xx, yy = lax.rem(data, 2), lax.rem(data // 2, 2), data // 4
        self.core, self.z = core, z
        flips = (2 - 4 * xx, 4 - 8 * yy)
        self.partner = (z, data + 1 - 2 * core)
        self.first = tuple((z, data + f) for f in flips)
        self.second = (self.first[1], self.first[0])
        self.c1, self.c2 = (xx, yy), (yy, xx)
        self.zs = [lax.rem(z + d, 4) for d in (1, 2, 3)]
        self.z_peers = [(zt, data) for zt in self.zs]

    def barrier(self, peers):
        sem = pltpu.get_barrier_semaphore()
        for peer in peers:
            pl.semaphore_signal(sem, inc=1, device_id=peer, device_id_type=MESH_ID)
        pl.semaphore_wait(sem, len(peers))


def remote(src, dst, send, recv, peer):
    return pltpu.make_async_remote_copy(src_ref=src, dst_ref=dst, send_sem=send, recv_sem=recv, device_id=peer, device_id_type=MESH_ID)


def last_kernel(count, x_ref, y_ref, vin_ref, vout_ref, w0, w1, o0, o1, lout, h_s, z_s, a_s, q_s, e_s, hT_s, gs0, gs1,
                d0, d1, r10, r11, r20, r21, r30, r31, s10, s11, s20, s21, s30, s31, nb0, nb1, wb0, wb1, lt, lr,
                w_sem, d_sem, r1_sem, r2_sem, r3_sem, az_sem, a2_sem, a1_sem, ad_sem,
                ds_sem, s1_sem, s2_sem, s3_sem, zs_sem, n_sem, a2s_sem, a1s_sem, ads_sem, l_sem, ls_sem):
    step = pl.program_id(0)
    me = Place()
    core, z = me.core, me.z
    gs, w, o = (gs0, gs1), (w0, w1), (o0, o1)
    dd, r1, r2, r3 = (d0, d1), (r10, r11), (r20, r21), (r30, r31)
    s1, s2, s3, nb, wb = (s10, s11), (s20, s21), (s30, s31), (nb0, nb1), (wb0, wb1)
    kinds = (0, 1)

    def quarter(kind):
        return (2 * me.c1[kind] + me.c2[kind]) * (ROWS[kind] // 4)

    def w_copy(l, k):
        n = ROWS[k] // 16
        return pltpu.make_async_copy(half_at(w[k], k, L - 1 - l, core, quarter(k) + z * n, n), wb[k].at[l], w_sem.at[l, k])

    def d_copy(l, k):
        slot = lax.rem(l, 3)
        return remote(half_at(gs[k], k, slot, 1 - core, 0, ROWS[k]), dd[k].at[l], ds_sem.at[slot, k], d_sem.at[l, k], me.partner)

    def r1_copy(l, k):
        slot = lax.rem(l, 2)
        return remote(s1[k].at[slot], r1[k].at[l], s1_sem.at[slot, k], r1_sem.at[l, k], me.first[k])

    def r2_copy(l, k):
        slot = lax.rem(l, 2)
        return remote(s2[k].at[slot], r2[k].at[l], s2_sem.at[slot, k], r2_sem.at[l, k], me.second[k])

    def r3_copy(l, k, j):
        slot, n = lax.rem(l, 2), ROWS[k] // 16
        return remote(s3[k].at[slot, pl.ds(al(me.zs[j] * n, 8), n)], r3[k].at[l, 2 - j], s3_sem.at[slot, k, j], r3_sem.at[l, k, 2 - j], me.z_peers[j])

    def piece(l, k, zi):
        n = ROWS[k] // 16
        return half_at(o[k], k, L - 1 - l, core, quarter(k) + zi * n, n)

    def az_copy(l, k, j):
        slot = lax.rem(l, 2)
        return remote(nb[k].at[slot], piece(l, k, z), zs_sem.at[slot, k, j], az_sem.at[l, k, 2 - j], me.z_peers[j])

    def n_copy(l, k):
        slot = lax.rem(l, 2)
        return pltpu.make_async_copy(nb[k].at[slot], piece(l, k, z), n_sem.at[slot, k])

    def gather(l, k, row, rows, send, recv, peer):
        part = half_at(o[k], k, L - 1 - l, core, row, rows)
        return remote(part, part, send.at[lax.rem(l, 2), k], recv.at[l, k], peer)

    def a2_copy(l, k):
        return gather(l, k, quarter(k), ROWS[k] // 4, a2s_sem, a2_sem, me.second[k])

    def a1_copy(l, k):
        return gather(l, k, me.c1[k] * (ROWS[k] // 2), ROWS[k] // 2, a1s_sem, a1_sem, me.first[k])

    def ad_copy(l, k):
        return gather(l, k, 0, ROWS[k], ads_sem, ad_sem, me.partner)

    def both(k, l, row, n):
        slot = lax.rem(l, 3)
        if k == 0:
            mine = gs[0][slot, pl.ds(row, n), pl.ds(al(core * COLS[0], 128), COLS[0])]
        else:
            mine = gs[1][slot, pl.ds(al(core * ROWS[1] + row, 16), n), :]
        return mine.astype(F32) + dd[k][l, pl.ds(row, n), :].astype(F32)

    def stage0(l, k):
        d_copy(l, k).wait_recv()

        @pl.when(l >= 2)
        def _():
            r1_copy(l - 2, k).wait_send()
        n, slot = ROWS[k] // 2, lax.rem(l, 2)
        base = (1 - me.c1[k]) * n

        def body(row):
            s1[k][slot, pl.ds(row, 16), :] = both(k, l, al(base + row, 16), 16)
        row_loop(n, 16, body)
        r1_copy(l, k).start()

    def stage1(l, k):
        r1_copy(l, k).wait_recv()

        @pl.when(l >= 2)
        def _():
            r2_copy(l - 2, k).wait_send()
        n, slot = ROWS[k] // 4, lax.rem(l, 2)
        in_half = (1 - me.c2[k]) * n
        base = me.c1[k] * 2 * n + in_half

        def body(row):
            s2[k][slot, pl.ds(row, 16), :] = both(k, l, al(base + row, 16), 16) + r1[k][l, pl.ds(al(in_half + row, 16), 16), :]
        row_loop(n, 16, body)
        r2_copy(l, k).start()

    def stage2(l, k):
        r2_copy(l, k).wait_recv()

        @pl.when(l >= 2)
        def _():
            for j in range(3):
                r3_copy(l - 2, k, j).wait_send()
        n, slot = ROWS[k] // 4, lax.rem(l, 2)
        in_half = me.c2[k] * n
        base = me.c1[k] * 2 * n + in_half

        def body(row):
            s3[k][slot, pl.ds(row, 16), :] = (both(k, l, al(base + row, 16), 16) + r1[k][l, pl.ds(al(in_half + row, 16), 16), :]) + r2[k][l, pl.ds(row, 16), :]
        row_loop(n, 16, body)
        for j in range(3):
            r3_copy(l, k, j).start()

    def stage3(l, k):
        for j in range(3):
            r3_copy(l, k, j).wait_recv()
        w_copy(l, k).wait()

        @pl.when(l >= 2)
        def _():
            for j in range(3):
                az_copy(l - 2, k, j).wait_send()
        n, slot = ROWS[k] // 16, lax.rem(l, 2)

        def body(row):
            rs = pl.ds(row, 8)
            tot = (s3[k][slot, pl.ds(al(z * n + row, 8), 8), :] + r3[k][l, 0, rs, :]) + (r3[k][l, 1, rs, :] + r3[k][l, 2, rs, :])
            nb[k][slot, rs, :] = wb[k][l, rs, :] - STEP_SIZE * (tot * (1.0 / count))
        row_loop(n, 8, body)
        n_copy(l, k).start()
        for j in range(3):
            az_copy(l, k, j).start()

    def stage4(l, k):
        n_copy(l, k).wait()
        for j in range(3):
            az_copy(l, k, j).wait_recv()

        @pl.when(l >= 2)
        def _():
            a2_copy(l - 2, k).wait_send()
        a2_copy(l, k).start()

    def stage5(l, k):
        a2_copy(l, k).wait_recv()

        @pl.when(l >= 2)
        def _():
            a1_copy(l - 2, k).wait_send()
        a1_copy(l, k).start()

    def stage6(l, k):
        a1_copy(l, k).wait_recv()

        @pl.when(l >= 2)
        def _():
            ad_copy(l - 2, k).wait_send()
        ad_copy(l, k).start()

    stages = (stage0, stage1, stage2, stage3, stage4, stage5, stage6)

    def loss_copy(i, peer, j):
        return remote(lt.at[i], lr.at[j], ls_sem.at[j], l_sem.at[j], peer)

    loss_hops = [[(me.partner, 0)], [(me.first[0], 1)], [(me.first[1], 2)], [(me.z_peers[j], 3 + j) for j in range(3)]]

    def loss_wait(i):
        for peer, j in loss_hops[i]:
            loss_copy(i, peer, j).wait()
        tot = lt[i]
        for _, j in loss_hops[i]:
            tot = tot + (lr[j] if i < 3 else lr[8 - j])
        return tot

    def start_all(l, _):
        for k in kinds:
            w_copy(l, k).start()
        return 0

    def loss_step(t):
        for i in range(5):
            @pl.when(t == i)
            def _(i=i):
                if i > 0:
                    tot = loss_wait(i - 1)
                    if i == 4:
                        lout[...] = tot * (1.0 / count)
                    else:
                        lt[i] = tot
                if i < 4:
                    for peer, j in loss_hops[i]:
                        loss_copy(i, peer, j).start()

    def tick(t, _):
        loss_step(t)

        @pl.when(t < L)
        def _():
            for k in kinds:
                d_copy(t, k).start()
        for s in reversed(range(STAGES)):
            l = t - s

            @pl.when(jnp.logical_and(l >= 0, l < L))
            def _(s=s, l=l):
                for k in kinds:
                    stages[s](l, k)
        return 0

    @pl.when(step == 0)
    def _():
        me.barrier([me.partner, me.first[0], me.first[1]] + me.z_peers)
        h_s[0] = x_ref[...]
        lax.fori_loop(0, L, start_all, 0)

    @pl.when(step < L)
    def _():
        h = h_s[step]
        for j in range(NT):
            cols = slice(j * FT, (j + 1) * FT)
            z_s[:, cols] = dot(h, vin_ref[0, :, cols]).astype(BF16)
            for rs, cs in chunks(j * FT):
                a_s[rs, cs] = gelu_only(z_s[rs, cs].astype(F32)).astype(BF16)
        h_s[step + 1] = (h.astype(F32) + dot(a_s[...], vout_ref[0])).astype(BF16)

    @pl.when(step == L - 1)
    def _():
        diff = h_s[L].astype(F32) - y_ref[...].astype(F32)
        lt[0] = jnp.full((8, 128), 0.5 * jnp.sum(diff * diff) / (T * D), F32)
        e_s[...] = (diff / (T * D)).astype(BF16)

    @pl.when(step >= L)
    def _():
        item = step - L
        slot = lax.rem(item, 3)
        lay = L - 1 - item

        @pl.when(item >= 3)
        def _():
            for k in kinds:
                d_copy(item - 3, k).wait_send()
        e, h = e_s[...], h_s[lay]
        hT_s[...] = h.T
        for j in range(NT):
            cols = slice(j * FT, (j + 1) * FT)
            z_s[:, cols] = dot(h, vin_ref[0, :, cols]).astype(BF16)
            q_s[:, cols] = dot(e, vout_ref[0, cols, :], 1, 1).astype(BF16)
            for rs, cs in chunks(j * FT):
                act, slope = gelu_both(z_s[rs, cs].astype(F32))
                a_s[rs, cs] = act.astype(BF16)
                q_s[rs, cs] = (slope * q_s[rs, cs].astype(F32)).astype(BF16)
            gs1[slot, cols, :] = dot(a_s[:, cols], e, 0, 0).astype(BF16)
            gs0[slot, :, cols] = dot(hT_s[...], q_s[:, cols]).astype(BF16)
        e_s[...] = (e.astype(F32) + dot(q_s[...], vin_ref[0], 1, 1)).astype(BF16)
        lax.fori_loop(item, jnp.where(item == L - 1, L + STAGES - 1, item + 1), tick, 0)

    @pl.when(step == 2 * L - 1)
    def _():
        def finish(l, _):
            for k in kinds:
                ad_copy(l, k).wait_recv()
            return 0
        lax.fori_loop(0, L, finish, 0)
        for l in (L - 3, L - 2, L - 1):
            for k in kinds:
                d_copy(l, k).wait_send()
        for l in (L - 2, L - 1):
            for k in kinds:
                r1_copy(l, k).wait_send()
                r2_copy(l, k).wait_send()
                for j in range(3):
                    r3_copy(l, k, j).wait_send()
                    az_copy(l, k, j).wait_send()
                a2_copy(l, k).wait_send()
                a1_copy(l, k).wait_send()
                ad_copy(l, k).wait_send()


def last_pass(count, x, y, vin, vout, w_in, w_out):
    def per_kind(lead, div, dtype):
        return [pltpu.VMEM(lead + (ROWS[k] // div, COLS[k]), dtype) for k in (0, 1)]
    dma = pltpu.SemaphoreType.DMA
    any_spec = pl.BlockSpec(memory_space=pl.ANY)
    lay = lambda s: jnp.where(s < L, s, 2 * L - 1 - s)
    scratch = ([pltpu.VMEM((L + 1, T, D), BF16)] + [pltpu.VMEM((T, F), BF16)] * 3 + [pltpu.VMEM((T, D), BF16), pltpu.VMEM((D, T), BF16)]
               + [pltpu.VMEM((3, D, F), BF16), pltpu.VMEM((3, F, D), BF16)]
               + per_kind((L,), 1, BF16) + per_kind((L,), 2, F32) + per_kind((L,), 4, F32)
               + per_kind((L, 3), 16, F32) + per_kind((2,), 2, F32) + per_kind((2,), 4, F32) + per_kind((2,), 4, F32)
               + per_kind((2,), 16, F32) + per_kind((L,), 16, F32) + [pltpu.VMEM((4, 8, 128), F32), pltpu.VMEM((6, 8, 128), F32)]
               + [dma((L, 2))] * 4 + [dma((L, 2, 3))] * 2 + [dma((L, 2))] * 3 + [dma((3, 2))]
               + [dma((2, 2))] * 2 + [dma((2, 2, 3))] * 2 + [dma((2, 2))] * 4 + [dma((6,))] * 2)
    return pl.pallas_call(
        functools.partial(last_kernel, count),
        grid=(2 * L,),
        in_specs=[
            pl.BlockSpec((T, D), lambda s: (0, 0), pipeline_mode=pl.Buffered(1)),
            pl.BlockSpec((T, D), lambda s: (0, 0), pipeline_mode=pl.Buffered(1)),
            pl.BlockSpec((1, D, F), lambda s: (lay(s), 0, 0)),
            pl.BlockSpec((1, F, D), lambda s: (lay(s), 0, 0)),
            any_spec,
            any_spec,
        ],
        out_specs=[any_spec, any_spec, pl.BlockSpec((8, 128), lambda s: (0, 0))],
        out_shape=[jax.ShapeDtypeStruct((L, D, F), F32), jax.ShapeDtypeStruct((L, F, D), F32), jax.ShapeDtypeStruct((8, 128), F32)],
        scratch_shapes=scratch,
        compiler_params=pltpu.CompilerParams(collective_id=1, has_side_effects=True, vmem_limit_bytes=67_000_000),
    )(x, y, vin, vout, w_in, w_out)


def ascent_kernel(group, a0, a1, b0, b1, w0, w1, t0, t1, oa0, oa1, ob0, ob1, pa0, pa1, pb0, pb1, wb0, wb1, tb0, tb1, nt,
                  o_sem, p_sem, ps_sem, w_sem, tl_sem, ts_sem, tr_sem, n_sem):
    me = Place()
    core = me.core
    src, w, t = ((a0, a1), (b0, b1)), (w0, w1), (t0, t1)
    own, peer = ((oa0, oa1), (ob0, ob1)), ((pa0, pa1), (pb0, pb1))
    wb, tb, kinds = (wb0, wb1), (tb0, tb1), (0, 1)
    me.barrier([me.partner])

    def own_copy(l, k, i):
        return pltpu.make_async_copy(half_at(src[i][k], k, l, core, 0, ROWS[k]), own[i][k].at[l], o_sem.at[l, k, i])

    def peer_copy(l, k, i):
        return remote(half_at(src[i][k], k, l, 1 - core, 0, ROWS[k]), peer[i][k].at[l], ps_sem.at[l, k, i], p_sem.at[l, k, i], me.partner)

    def w_copy(l, k):
        slot = lax.rem(l, 2)
        return pltpu.make_async_copy(half_at(w[k], k, l, core, 0, ROWS[k]), wb[k].at[slot], w_sem.at[slot, k])

    def t_half(l, k):
        return half_at(t[k], k, l, core, 0, ROWS[k])

    def t_local(l, k):
        slot = lax.rem(l, 2)
        return pltpu.make_async_copy(tb[k].at[slot], t_half(l, k), tl_sem.at[slot, k])

    def t_send(l, k):
        slot = lax.rem(l, 2)
        return remote(tb[k].at[slot], t_half(l, k), ts_sem.at[slot, k], tr_sem.at[l, k], me.partner)

    def mean_rows(l, k, row):
        rs = pl.ds(row, 16)
        f = lambda ref: ref[l, rs, :].astype(F32)
        return ((f(own[0][k]) + f(own[1][k])) + (f(peer[0][k]) + f(peer[1][k]))) * (1.0 / group)

    def start_all(l, _):
        for k in kinds:
            for i in range(2):
                peer_copy(l, k, i).start()
                own_copy(l, k, i).start()
        return 0
    lax.fori_loop(0, L, start_all, 0)
    for l in range(2):
        for k in kinds:
            w_copy(l, k).start()

    def square_layer(l, acc):
        for k in kinds:
            for i in range(2):
                own_copy(l, k, i).wait()
                peer_copy(l, k, i).wait_recv()

            def body(i, tot, k=k):
                g = mean_rows(l, k, al(i * 16, 16))
                sq = g * g
                parts = [sq[r:r + 8, c:c + 128] for r in (0, 8) for c in range(0, COLS[k], 128)]
                while len(parts) > 1:
                    parts = [u + v for u, v in zip(parts[::2], parts[1::2])] + parts[len(parts) & ~1:]
                return tot + parts[0]
            acc = lax.fori_loop(0, ROWS[k] // 16, body, acc)
        return acc
    nt[0] = lax.fori_loop(0, L, square_layer, jnp.zeros((8, 128), F32))
    norm_copy = remote(nt.at[0], nt.at[1], n_sem.at[0], n_sem.at[1], me.partner)
    norm_copy.start()
    norm_copy.wait()
    total = jnp.sum(jnp.sum(nt[0] + nt[1], axis=0, keepdims=True), axis=1, keepdims=True)
    scale = (RHO_SCALE * D ** 0.5) / jnp.sqrt(total)

    def move_layer(l, _):
        for k in kinds:
            slot = lax.rem(l, 2)
            w_copy(l, k).wait()

            @pl.when(l >= 2)
            def _(k=k):
                t_local(l - 2, k).wait()
                t_send(l - 2, k).wait_send()

            def body(row, k=k, slot=slot):
                rs = pl.ds(row, 16)
                tb[k][slot, rs, :] = (wb[k][slot, rs, :] + scale * mean_rows(l, k, row)).astype(BF16)
            row_loop(ROWS[k], 16, body)
            t_send(l, k).start()
            t_local(l, k).start()

            @pl.when(l < L - 2)
            def _(k=k):
                w_copy(l + 2, k).start()
        return 0
    lax.fori_loop(0, L, move_layer, 0)

    def finish(l, _):
        for k in kinds:
            t_send(l, k).wait_recv()
            for i in range(2):
                peer_copy(l, k, i).wait_send()
        return 0
    lax.fori_loop(0, L, finish, 0)
    for l in (L - 2, L - 1):
        for k in kinds:
            t_local(l, k).wait()
            t_send(l, k).wait_send()


def ascent(group, first, second, w_in, w_out):
    def per_kind(lead, dtype):
        return [pltpu.VMEM((lead, ROWS[k], COLS[k]), dtype) for k in (0, 1)]
    dma = pltpu.SemaphoreType.DMA
    any_spec = pl.BlockSpec(memory_space=pl.ANY)
    scratch = (per_kind(L, BF16) * 4 + per_kind(2, F32) + per_kind(2, BF16) + [pltpu.VMEM((2, 8, 128), F32)]
               + [dma((L, 2, 2))] * 3 + [dma((2, 2))] * 3 + [dma((L, 2)), dma((2,))])
    return pl.pallas_call(
        functools.partial(ascent_kernel, group),
        in_specs=[any_spec] * 6,
        out_specs=[any_spec] * 2,
        out_shape=[jax.ShapeDtypeStruct((L, D, F), BF16), jax.ShapeDtypeStruct((L, F, D), BF16)],
        scratch_shapes=scratch,
        compiler_params=pltpu.CompilerParams(collective_id=2, has_side_effects=True, vmem_limit_bytes=60 * 2**20),
    )(*first, *second, w_in, w_out)


def move_pairs(sub_size, data_size, flip):
    pairs = []
    for shard in range(sub_size):
        for data_idx in range(data_size):
            group = data_idx % 2
            chip = 2 * group + ((shard + flip) % 2)
            pairs.append((shard * data_size + data_idx, chip * data_size + data_idx - group + shard // 2))
    return pairs


def solution(mesh):
    sub_size, data_size = mesh.shape["sub"], mesh.shape["data"]
    dev_count = sub_size * data_size
    axes = ("sub", "data")

    def device_step(x_blk, y_blk, w_in, w_out):
        tok = jnp.stack([x_blk.reshape(T, D), y_blk.reshape(T, D)])
        own = lax.ppermute(tok, axes, move_pairs(sub_size, data_size, 0))
        other = lax.ppermute(tok, axes, move_pairs(sub_size, data_size, 1))
        v_in, v_out = w_in.astype(BF16), w_out.astype(BF16)
        first = run_pass(own[0], own[1], v_in, v_out)[:2]
        second = run_pass(other[0], other[1], v_in, v_out)[:2]
        t_in, t_out = ascent(sub_size, first, second, w_in, w_out)
        new_in, new_out, loss_all = last_pass(dev_count, own[0], own[1], t_in, t_out, w_in, w_out)
        return new_in, new_out, loss_all[0, 0]

    batch_spec = P(("data", "sub"))
    return jax.shard_map(device_step, mesh=mesh, in_specs=(batch_spec, batch_spec, P(), P()), out_specs=(P(), P(), P()), check_vma=False)
```

```python
import jax, jax.numpy as jnp, functools
from jax import lax
from jax.experimental import pallas as pl
from jax.experimental.pallas import tpu as pltpu
from jax.sharding import PartitionSpec as P

F32, BF16 = jnp.float32, jnp.bfloat16
RHO_SCALE = 0.1
STEP_SIZE = 1.0
L, T, D, F = 8, 784, 384, 1536
FT = 256
NT = F // FT
RC, CC = 16, 256
SQRT_HALF = 0.5 ** 0.5
INV_SQRT_2PI = 0.3989422804014327


def gelu_only(z):
    return z * (0.5 + 0.5 * lax.erf(z * SQRT_HALF))


def gelu_both(z):
    cdf = 0.5 + 0.5 * lax.erf(z * SQRT_HALF)
    pdf = INV_SQRT_2PI * jnp.exp(-0.5 * (z * z))
    return z * cdf, cdf + z * pdf


def chunks(col0):
    for c in range(FT // CC):
        for r in range(T // RC):
            yield slice(r * RC, (r + 1) * RC), slice(col0 + c * CC, col0 + (c + 1) * CC)


def dot(a, b, ca=1, cb=0):
    return lax.dot_general(a, b, (((ca,), (cb,)), ((), ())), preferred_element_type=F32)


def pass_kernel(x_ref, y_ref, vin_ref, vout_ref, gin_ref, gout_ref, loss_ref, h_s, z_s, a_s, q_s, e_s, hT_s):
    step = pl.program_id(0)

    @pl.when(step == 0)
    def _():
        h_s[0] = x_ref[...]

    @pl.when(step < L)
    def _():
        lay = step
        z_l = z_s.at[lay]
        h = h_s[lay]
        def pre(j):
            cols = slice(j * FT, (j + 1) * FT)
            z_l[:, cols] = dot(h, vin_ref[0, :, cols]).astype(BF16)

        pre(0)
        for j in range(NT):
            if j + 1 < NT:
                pre(j + 1)
            for rs, cs in chunks(j * FT):
                a_s[rs, cs] = gelu_only(z_l[rs, cs].astype(F32)).astype(BF16)
        out = (h.astype(F32) + dot(a_s[...], vout_ref[0])).astype(BF16)
        h_s[lay + 1] = out

    @pl.when(step == L - 1)
    def _():
        diff = h_s[L].astype(F32) - y_ref[...].astype(F32)
        loss_ref[0, 0] = 0.5 * jnp.sum(diff * diff) / (T * D)
        e_s[...] = (diff / (T * D)).astype(BF16)

    @pl.when(step >= L)
    def _():
        lay = 2 * L - 1 - step
        z_l = z_s.at[lay]
        e = e_s[...]
        hT_s[...] = h_s[lay].T
        def up(j):
            cols = slice(j * FT, (j + 1) * FT)
            q_s[:, cols] = dot(e, vout_ref[0, cols, :], 1, 1).astype(BF16)

        up(0)
        for j in range(NT):
            if j + 1 < NT:
                up(j + 1)
            for rs, cs in chunks(j * FT):
                act, slope = gelu_both(z_l[rs, cs].astype(F32))
                a_s[rs, cs] = act.astype(BF16)
                q_s[rs, cs] = (slope * q_s[rs, cs].astype(F32)).astype(BF16)
        gout_ref[0] = dot(a_s[...], e, 0, 0).astype(BF16)
        gin_ref[0] = dot(hT_s[...], q_s[...]).astype(BF16)
        e_s[...] = (e.astype(F32) + dot(q_s[...], vin_ref[0], 1, 1)).astype(BF16)


def swap_pass_kernel(x_ref, y_ref, vin_ref, vout_ref, a0, a1, gin_ref, gout_ref, loss_ref, p0, p1, h_s, z_s, a_s, q_s, e_s, hT_s, s_sem, r_sem):
    me = Place()
    src, dst = (a0, a1), (p0, p1)

    def copy(l, k):
        return remote(half_at(src[k], k, l, 1 - me.core, 0, ROWS[k]), dst[k].at[l], s_sem.at[l, k], r_sem.at[l, k], me.partner)

    @pl.when(pl.program_id(0) == 0)
    def _():
        me.barrier([me.partner])

        def begin(l, _):
            for k in (0, 1):
                copy(l, k).start()
            return 0
        lax.fori_loop(0, L, begin, 0)
    pass_kernel(x_ref, y_ref, vin_ref, vout_ref, gin_ref, gout_ref, loss_ref, h_s, z_s, a_s, q_s, e_s, hT_s)

    @pl.when(pl.program_id(0) == 2 * L - 1)
    def _():
        def end(l, _):
            for k in (0, 1):
                copy(l, k).wait()
            return 0
        lax.fori_loop(0, L, end, 0)


def run_pass(x, y, vin, vout, earlier=()):
    lay = lambda s: jnp.where(s < L, s, 2 * L - 1 - s)
    glay = lambda s: jnp.where(s < L, L - 1, 2 * L - 1 - s)
    any_spec = pl.BlockSpec(memory_space=pl.ANY)
    extra = [any_spec] * len(earlier)
    landed = [jax.ShapeDtypeStruct((L, ROWS[k], COLS[k]), BF16) for k in range(len(earlier))]
    sems = [pltpu.SemaphoreType.DMA((L, 2))] * len(earlier)
    more = dict(collective_id=3, has_side_effects=True) if earlier else {}
    return pl.pallas_call(
        swap_pass_kernel if earlier else pass_kernel,
        grid=(2 * L,),
        in_specs=[
            pl.BlockSpec((T, D), lambda s: (0, 0)),
            pl.BlockSpec((T, D), lambda s: (0, 0)),
            pl.BlockSpec((1, D, F), lambda s: (lay(s), 0, 0)),
            pl.BlockSpec((1, F, D), lambda s: (lay(s), 0, 0)),
        ] + extra,
        out_specs=[
            pl.BlockSpec((1, D, F), lambda s: (glay(s), 0, 0)),
            pl.BlockSpec((1, F, D), lambda s: (glay(s), 0, 0)),
            pl.BlockSpec(memory_space=pltpu.SMEM),
        ] + extra,
        out_shape=[
            jax.ShapeDtypeStruct((L, D, F), BF16),
            jax.ShapeDtypeStruct((L, F, D), BF16),
            jax.ShapeDtypeStruct((1, 1), F32),
        ] + landed,
        scratch_shapes=[
            pltpu.VMEM((L + 1, T, D), BF16),
            pltpu.VMEM((L, T, F), BF16),
            pltpu.VMEM((T, F), BF16),
            pltpu.VMEM((T, F), BF16),
            pltpu.VMEM((T, D), BF16),
            pltpu.VMEM((D, T), BF16),
        ] + sems,
        compiler_params=pltpu.CompilerParams(vmem_limit_bytes=60 * 2**20, **more),
        cost_estimate=pl.CostEstimate(flops=L * 12 * T * D * F, bytes_accessed=4 * L * D * F * 2, transcendentals=0),
    )(x, y, vin, vout, *earlier)


ROWS = (384, 768)
COLS = (768, 384)
STAGES = 7
MESH_ID = pl.DeviceIdType.MESH


def al(v, n):
    return pl.multiple_of(v, n)


def half_at(ref, kind, lay, core, row, rows):
    if kind == 0:
        return ref.at[lay, pl.ds(al(row, 8), rows), pl.ds(al(core * COLS[0], 128), COLS[0])]
    return ref.at[lay, pl.ds(al(core * ROWS[1] + row, 8), rows), :]


def row_loop(rows, block, body):
    def step(i, _):
        body(al(i * block, block))
        return 0
    lax.fori_loop(0, rows // block, step, 0)


class Place:
    def __init__(self):
        z, data = lax.axis_index("sub"), lax.axis_index("data")
        core, xx, yy = lax.rem(data, 2), lax.rem(data // 2, 2), data // 4
        self.core, self.z = core, z
        flips = (2 - 4 * xx, 4 - 8 * yy)
        self.partner = (z, data + 1 - 2 * core)
        self.first = tuple((z, data + f) for f in flips)
        self.second = (self.first[1], self.first[0])
        self.c1, self.c2 = (xx, yy), (yy, xx)
        self.zs = [lax.rem(z + d, 4) for d in (1, 2, 3)]
        self.z_peers = [(zt, data) for zt in self.zs]

    def barrier(self, peers):
        sem = pltpu.get_barrier_semaphore()
        for peer in peers:
            pl.semaphore_signal(sem, inc=1, device_id=peer, device_id_type=MESH_ID)
        pl.semaphore_wait(sem, len(peers))


def remote(src, dst, send, recv, peer):
    return pltpu.make_async_remote_copy(src_ref=src, dst_ref=dst, send_sem=send, recv_sem=recv, device_id=peer, device_id_type=MESH_ID)


def last_kernel(count, x_ref, y_ref, vin_ref, vout_ref, w0, w1, o0, o1, lout, h_s, z_s, a_s, q_s, e_s, hT_s, gs0, gs1,
                d0, d1, r10, r11, r20, r21, r30, r31, s10, s11, s20, s21, s30, s31, nb0, nb1, wb0, wb1, lt, lr,
                w_sem, d_sem, r1_sem, r2_sem, r3_sem, az_sem, a2_sem, a1_sem, ad_sem,
                ds_sem, s1_sem, s2_sem, s3_sem, zs_sem, n_sem, a2s_sem, a1s_sem, ads_sem, l_sem, ls_sem):
    step = pl.program_id(0)
    me = Place()
    core, z = me.core, me.z
    gs, w, o = (gs0, gs1), (w0, w1), (o0, o1)
    dd, r1, r2, r3 = (d0, d1), (r10, r11), (r20, r21), (r30, r31)
    s1, s2, s3, nb, wb = (s10, s11), (s20, s21), (s30, s31), (nb0, nb1), (wb0, wb1)
    kinds = (0, 1)

    def quarter(kind):
        return (2 * me.c1[kind] + me.c2[kind]) * (ROWS[kind] // 4)

    def w_copy(l, k):
        n = ROWS[k] // 16
        return pltpu.make_async_copy(half_at(w[k], k, L - 1 - l, core, quarter(k) + z * n, n), wb[k].at[l], w_sem.at[l, k])

    def d_copy(l, k):
        slot = lax.rem(l, 3)
        return remote(half_at(gs[k], k, slot, 1 - core, 0, ROWS[k]), dd[k].at[l], ds_sem.at[slot, k], d_sem.at[l, k], me.partner)

    def r1_copy(l, k):
        slot = lax.rem(l, 2)
        return remote(s1[k].at[slot], r1[k].at[l], s1_sem.at[slot, k], r1_sem.at[l, k], me.first[k])

    def r2_copy(l, k):
        slot = lax.rem(l, 2)
        return remote(s2[k].at[slot], r2[k].at[l], s2_sem.at[slot, k], r2_sem.at[l, k], me.second[k])

    def r3_copy(l, k, j):
        slot, n = lax.rem(l, 2), ROWS[k] // 16
        return remote(s3[k].at[slot, pl.ds(al(me.zs[j] * n, 8), n)], r3[k].at[l, 2 - j], s3_sem.at[slot, k, j], r3_sem.at[l, k, 2 - j], me.z_peers[j])

    def piece(l, k, zi):
        n = ROWS[k] // 16
        return half_at(o[k], k, L - 1 - l, core, quarter(k) + zi * n, n)

    def az_copy(l, k, j):
        slot = lax.rem(l, 2)
        return remote(nb[k].at[slot], piece(l, k, z), zs_sem.at[slot, k, j], az_sem.at[l, k, 2 - j], me.z_peers[j])

    def n_copy(l, k):
        slot = lax.rem(l, 2)
        return pltpu.make_async_copy(nb[k].at[slot], piece(l, k, z), n_sem.at[slot, k])

    def gather(l, k, row, rows, send, recv, peer):
        part = half_at(o[k], k, L - 1 - l, core, row, rows)
        return remote(part, part, send.at[lax.rem(l, 2), k], recv.at[l, k], peer)

    def a2_copy(l, k):
        return gather(l, k, quarter(k), ROWS[k] // 4, a2s_sem, a2_sem, me.second[k])

    def a1_copy(l, k):
        return gather(l, k, me.c1[k] * (ROWS[k] // 2), ROWS[k] // 2, a1s_sem, a1_sem, me.first[k])

    def ad_copy(l, k):
        return gather(l, k, 0, ROWS[k], ads_sem, ad_sem, me.partner)

    def both(k, l, row, n):
        slot = lax.rem(l, 3)
        if k == 0:
            mine = gs[0][slot, pl.ds(row, n), pl.ds(al(core * COLS[0], 128), COLS[0])]
        else:
            mine = gs[1][slot, pl.ds(al(core * ROWS[1] + row, 16), n), :]
        return mine.astype(F32) + dd[k][l, pl.ds(row, n), :].astype(F32)

    def stage0(l, k):
        d_copy(l, k).wait_recv()

        @pl.when(l >= 2)
        def _():
            r1_copy(l - 2, k).wait_send()
        n, slot = ROWS[k] // 2, lax.rem(l, 2)
        base = (1 - me.c1[k]) * n

        def body(row):
            s1[k][slot, pl.ds(row, 16), :] = both(k, l, al(base + row, 16), 16)
        row_loop(n, 16, body)
        r1_copy(l, k).start()

    def stage1(l, k):
        r1_copy(l, k).wait_recv()

        @pl.when(l >= 2)
        def _():
            r2_copy(l - 2, k).wait_send()
        n, slot = ROWS[k] // 4, lax.rem(l, 2)
        in_half = (1 - me.c2[k]) * n
        base = me.c1[k] * 2 * n + in_half

        def body(row):
            s2[k][slot, pl.ds(row, 16), :] = both(k, l, al(base + row, 16), 16) + r1[k][l, pl.ds(al(in_half + row, 16), 16), :]
        row_loop(n, 16, body)
        r2_copy(l, k).start()

    def stage2(l, k):
        r2_copy(l, k).wait_recv()

        @pl.when(l >= 2)
        def _():
            for j in range(3):
                r3_copy(l - 2, k, j).wait_send()
        n, slot = ROWS[k] // 4, lax.rem(l, 2)
        in_half = me.c2[k] * n
        base = me.c1[k] * 2 * n + in_half

        def body(row):
            s3[k][slot, pl.ds(row, 16), :] = (both(k, l, al(base + row, 16), 16) + r1[k][l, pl.ds(al(in_half + row, 16), 16), :]) + r2[k][l, pl.ds(row, 16), :]
        row_loop(n, 16, body)
        for j in range(3):
            r3_copy(l, k, j).start()

    def stage3(l, k):
        for j in range(3):
            r3_copy(l, k, j).wait_recv()
        w_copy(l, k).wait()

        @pl.when(l >= 2)
        def _():
            for j in range(3):
                az_copy(l - 2, k, j).wait_send()
        n, slot = ROWS[k] // 16, lax.rem(l, 2)

        def body(row):
            rs = pl.ds(row, 8)
            tot = (s3[k][slot, pl.ds(al(z * n + row, 8), 8), :] + r3[k][l, 0, rs, :]) + (r3[k][l, 1, rs, :] + r3[k][l, 2, rs, :])
            nb[k][slot, rs, :] = wb[k][l, rs, :] - STEP_SIZE * (tot * (1.0 / count))
        row_loop(n, 8, body)
        n_copy(l, k).start()
        for j in range(3):
            az_copy(l, k, j).start()

    def stage4(l, k):
        n_copy(l, k).wait()
        for j in range(3):
            az_copy(l, k, j).wait_recv()

        @pl.when(l >= 2)
        def _():
            a2_copy(l - 2, k).wait_send()
        a2_copy(l, k).start()

    def stage5(l, k):
        a2_copy(l, k).wait_recv()

        @pl.when(l >= 2)
        def _():
            a1_copy(l - 2, k).wait_send()
        a1_copy(l, k).start()

    def stage6(l, k):
        a1_copy(l, k).wait_recv()

        @pl.when(l >= 2)
        def _():
            ad_copy(l - 2, k).wait_send()
        ad_copy(l, k).start()

    stages = (stage0, stage1, stage2, stage3, stage4, stage5, stage6)

    def loss_copy(i, peer, j):
        return remote(lt.at[i], lr.at[j], ls_sem.at[j], l_sem.at[j], peer)

    loss_hops = [[(me.partner, 0)], [(me.first[0], 1)], [(me.first[1], 2)], [(me.z_peers[j], 3 + j) for j in range(3)]]

    def loss_wait(i):
        for peer, j in loss_hops[i]:
            loss_copy(i, peer, j).wait()
        tot = lt[i]
        for _, j in loss_hops[i]:
            tot = tot + (lr[j] if i < 3 else lr[8 - j])
        return tot

    def start_all(l, _):
        for k in kinds:
            w_copy(l, k).start()
        return 0

    def loss_step(t):
        for i in range(5):
            @pl.when(t == i)
            def _(i=i):
                if i > 0:
                    tot = loss_wait(i - 1)
                    if i == 4:
                        lout[...] = tot * (1.0 / count)
                    else:
                        lt[i] = tot
                if i < 4:
                    for peer, j in loss_hops[i]:
                        loss_copy(i, peer, j).start()

    def tick(t, _):
        loss_step(t)

        @pl.when(t < L)
        def _():
            for k in kinds:
                d_copy(t, k).start()
        for s in reversed(range(STAGES)):
            l = t - s

            @pl.when(jnp.logical_and(l >= 0, l < L))
            def _(s=s, l=l):
                for k in kinds:
                    stages[s](l, k)
        return 0

    @pl.when(step == 0)
    def _():
        me.barrier([me.partner, me.first[0], me.first[1]] + me.z_peers)
        h_s[0] = x_ref[...]
        lax.fori_loop(0, L, start_all, 0)

    @pl.when(step < L)
    def _():
        h = h_s[step]
        for j in range(NT):
            cols = slice(j * FT, (j + 1) * FT)
            z_s[:, cols] = dot(h, vin_ref[0, :, cols]).astype(BF16)
            for rs, cs in chunks(j * FT):
                a_s[rs, cs] = gelu_only(z_s[rs, cs].astype(F32)).astype(BF16)
        h_s[step + 1] = (h.astype(F32) + dot(a_s[...], vout_ref[0])).astype(BF16)

    @pl.when(step == L - 1)
    def _():
        diff = h_s[L].astype(F32) - y_ref[...].astype(F32)
        lt[0] = jnp.full((8, 128), 0.5 * jnp.sum(diff * diff) / (T * D), F32)
        e_s[...] = (diff / (T * D)).astype(BF16)

    @pl.when(step >= L)
    def _():
        item = step - L
        slot = lax.rem(item, 3)
        lay = L - 1 - item

        @pl.when(item >= 3)
        def _():
            for k in kinds:
                d_copy(item - 3, k).wait_send()
        e, h = e_s[...], h_s[lay]
        hT_s[...] = h.T
        for j in range(NT):
            cols = slice(j * FT, (j + 1) * FT)
            z_s[:, cols] = dot(h, vin_ref[0, :, cols]).astype(BF16)
            q_s[:, cols] = dot(e, vout_ref[0, cols, :], 1, 1).astype(BF16)
            for rs, cs in chunks(j * FT):
                act, slope = gelu_both(z_s[rs, cs].astype(F32))
                a_s[rs, cs] = act.astype(BF16)
                q_s[rs, cs] = (slope * q_s[rs, cs].astype(F32)).astype(BF16)
            gs1[slot, cols, :] = dot(a_s[:, cols], e, 0, 0).astype(BF16)
            gs0[slot, :, cols] = dot(hT_s[...], q_s[:, cols]).astype(BF16)
        e_s[...] = (e.astype(F32) + dot(q_s[...], vin_ref[0], 1, 1)).astype(BF16)
        lax.fori_loop(item, jnp.where(item == L - 1, L + STAGES - 1, item + 1), tick, 0)

    @pl.when(step == 2 * L - 1)
    def _():
        def finish(l, _):
            for k in kinds:
                ad_copy(l, k).wait_recv()
            return 0
        lax.fori_loop(0, L, finish, 0)
        for l in (L - 3, L - 2, L - 1):
            for k in kinds:
                d_copy(l, k).wait_send()
        for l in (L - 2, L - 1):
            for k in kinds:
                r1_copy(l, k).wait_send()
                r2_copy(l, k).wait_send()
                for j in range(3):
                    r3_copy(l, k, j).wait_send()
                    az_copy(l, k, j).wait_send()
                a2_copy(l, k).wait_send()
                a1_copy(l, k).wait_send()
                ad_copy(l, k).wait_send()


def last_pass(count, x, y, vin, vout, w_in, w_out):
    def per_kind(lead, div, dtype):
        return [pltpu.VMEM(lead + (ROWS[k] // div, COLS[k]), dtype) for k in (0, 1)]
    dma = pltpu.SemaphoreType.DMA
    any_spec = pl.BlockSpec(memory_space=pl.ANY)
    lay = lambda s: jnp.where(s < L, s, 2 * L - 1 - s)
    scratch = ([pltpu.VMEM((L + 1, T, D), BF16)] + [pltpu.VMEM((T, F), BF16)] * 3 + [pltpu.VMEM((T, D), BF16), pltpu.VMEM((D, T), BF16)]
               + [pltpu.VMEM((3, D, F), BF16), pltpu.VMEM((3, F, D), BF16)]
               + per_kind((L,), 1, BF16) + per_kind((L,), 2, F32) + per_kind((L,), 4, F32)
               + per_kind((L, 3), 16, F32) + per_kind((2,), 2, F32) + per_kind((2,), 4, F32) + per_kind((2,), 4, F32)
               + per_kind((2,), 16, F32) + per_kind((L,), 16, F32) + [pltpu.VMEM((4, 8, 128), F32), pltpu.VMEM((6, 8, 128), F32)]
               + [dma((L, 2))] * 4 + [dma((L, 2, 3))] * 2 + [dma((L, 2))] * 3 + [dma((3, 2))]
               + [dma((2, 2))] * 2 + [dma((2, 2, 3))] * 2 + [dma((2, 2))] * 4 + [dma((6,))] * 2)
    return pl.pallas_call(
        functools.partial(last_kernel, count),
        grid=(2 * L,),
        in_specs=[
            pl.BlockSpec((T, D), lambda s: (0, 0), pipeline_mode=pl.Buffered(1)),
            pl.BlockSpec((T, D), lambda s: (0, 0), pipeline_mode=pl.Buffered(1)),
            pl.BlockSpec((1, D, F), lambda s: (lay(s), 0, 0)),
            pl.BlockSpec((1, F, D), lambda s: (lay(s), 0, 0)),
            any_spec,
            any_spec,
        ],
        out_specs=[any_spec, any_spec, pl.BlockSpec((8, 128), lambda s: (0, 0))],
        out_shape=[jax.ShapeDtypeStruct((L, D, F), F32), jax.ShapeDtypeStruct((L, F, D), F32), jax.ShapeDtypeStruct((8, 128), F32)],
        scratch_shapes=scratch,
        compiler_params=pltpu.CompilerParams(collective_id=1, has_side_effects=True, vmem_limit_bytes=67_000_000),
    )(x, y, vin, vout, w_in, w_out)


def ascent_kernel(group, a0, a1, b0, b1, h0, h1, w0, w1, t0, t1, oa0, oa1, ob0, ob1, pa0, pa1, pb0, pb1, wb0, wb1, tb0, tb1, nt,
                  o_sem, p_sem, ps_sem, w_sem, tl_sem, ts_sem, tr_sem, n_sem):
    me = Place()
    core = me.core
    src, w, t = ((a0, a1), (b0, b1)), (w0, w1), (t0, t1)
    own, peer = ((oa0, oa1), (ob0, ob1)), ((pa0, pa1), (pb0, pb1))
    wb, tb, kinds = (wb0, wb1), (tb0, tb1), (0, 1)
    me.barrier([me.partner])

    def own_copy(l, k, i):
        return pltpu.make_async_copy(half_at(src[i][k], k, l, core, 0, ROWS[k]), own[i][k].at[l], o_sem.at[l, k, i])

    def peer_copy(l, k, i):
        if i == 0:
            return pltpu.make_async_copy((h0, h1)[k].at[l], peer[0][k].at[l], p_sem.at[l, k, 0])
        return remote(half_at(src[i][k], k, l, 1 - core, 0, ROWS[k]), peer[i][k].at[l], ps_sem.at[l, k, i], p_sem.at[l, k, i], me.partner)

    def w_copy(l, k):
        slot = lax.rem(l, 2)
        return pltpu.make_async_copy(half_at(w[k], k, l, core, 0, ROWS[k]), wb[k].at[slot], w_sem.at[slot, k])

    def t_half(l, k):
        return half_at(t[k], k, l, core, 0, ROWS[k])

    def t_local(l, k):
        slot = lax.rem(l, 2)
        return pltpu.make_async_copy(tb[k].at[slot], t_half(l, k), tl_sem.at[slot, k])

    def t_send(l, k):
        slot = lax.rem(l, 2)
        return remote(tb[k].at[slot], t_half(l, k), ts_sem.at[slot, k], tr_sem.at[l, k], me.partner)

    def mean_rows(l, k, row):
        rs = pl.ds(row, 16)
        f = lambda ref: ref[l, rs, :].astype(F32)
        return ((f(own[0][k]) + f(own[1][k])) + (f(peer[0][k]) + f(peer[1][k]))) * (1.0 / group)

    def start_all(l, _):
        for k in kinds:
            for i in (1, 0):
                peer_copy(l, k, i).start()
                own_copy(l, k, i).start()
        return 0
    lax.fori_loop(0, L, start_all, 0)
    for l in range(2):
        for k in kinds:
            w_copy(l, k).start()

    def square_layer(l, acc):
        for k in kinds:
            own_copy(l, k, 0).wait()
            own_copy(l, k, 1).wait()
            peer_copy(l, k, 0).wait()
            peer_copy(l, k, 1).wait_recv()

            def body(i, tot, k=k):
                g = mean_rows(l, k, al(i * 16, 16))
                sq = g * g
                parts = [sq[r:r + 8, c:c + 128] for r in (0, 8) for c in range(0, COLS[k], 128)]
                while len(parts) > 1:
                    parts = [u + v for u, v in zip(parts[::2], parts[1::2])] + parts[len(parts) & ~1:]
                return tot + parts[0]
            acc = lax.fori_loop(0, ROWS[k] // 16, body, acc)
        return acc
    nt[0] = lax.fori_loop(0, L, square_layer, jnp.zeros((8, 128), F32))
    norm_copy = remote(nt.at[0], nt.at[1], n_sem.at[0], n_sem.at[1], me.partner)
    norm_copy.start()
    norm_copy.wait()
    total = jnp.sum(jnp.sum(nt[0] + nt[1], axis=0, keepdims=True), axis=1, keepdims=True)
    scale = (RHO_SCALE * D ** 0.5) / jnp.sqrt(total)

    def move_layer(l, _):
        for k in kinds:
            slot = lax.rem(l, 2)
            w_copy(l, k).wait()

            @pl.when(l >= 2)
            def _(k=k):
                t_local(l - 2, k).wait()
                t_send(l - 2, k).wait_send()

            def body(row, k=k, slot=slot):
                rs = pl.ds(row, 16)
                tb[k][slot, rs, :] = (wb[k][slot, rs, :] + scale * mean_rows(l, k, row)).astype(BF16)
            row_loop(ROWS[k], 16, body)
            t_send(l, k).start()
            t_local(l, k).start()

            @pl.when(l < L - 2)
            def _(k=k):
                w_copy(l + 2, k).start()
        return 0
    lax.fori_loop(0, L, move_layer, 0)

    def finish(l, _):
        for k in kinds:
            t_send(l, k).wait_recv()
            peer_copy(l, k, 1).wait_send()
        return 0
    lax.fori_loop(0, L, finish, 0)
    for l in (L - 2, L - 1):
        for k in kinds:
            t_local(l, k).wait()
            t_send(l, k).wait_send()


def ascent(group, first, second, landed, w_in, w_out):
    def per_kind(lead, dtype):
        return [pltpu.VMEM((lead, ROWS[k], COLS[k]), dtype) for k in (0, 1)]
    dma = pltpu.SemaphoreType.DMA
    any_spec = pl.BlockSpec(memory_space=pl.ANY)
    scratch = (per_kind(L, BF16) * 4 + per_kind(2, F32) + per_kind(2, BF16) + [pltpu.VMEM((2, 8, 128), F32)]
               + [dma((L, 2, 2))] * 3 + [dma((2, 2))] * 3 + [dma((L, 2)), dma((2,))])
    return pl.pallas_call(
        functools.partial(ascent_kernel, group),
        in_specs=[any_spec] * 8,
        out_specs=[any_spec] * 2,
        out_shape=[jax.ShapeDtypeStruct((L, D, F), BF16), jax.ShapeDtypeStruct((L, F, D), BF16)],
        scratch_shapes=scratch,
        compiler_params=pltpu.CompilerParams(collective_id=2, has_side_effects=True, vmem_limit_bytes=60 * 2**20),
    )(*first, *second, *landed, w_in, w_out)


def move_pairs(sub_size, data_size, flip):
    pairs = []
    for shard in range(sub_size):
        for data_idx in range(data_size):
            group = data_idx % 2
            chip = 2 * ((shard // 2 + flip) % 2) + group
            pairs.append((shard * data_size + data_idx, chip * data_size + data_idx - group + shard % 2))
    return pairs


def solution(mesh):
    sub_size, data_size = mesh.shape["sub"], mesh.shape["data"]
    dev_count = sub_size * data_size
    axes = ("sub", "data")

    def device_step(x_blk, y_blk, w_in, w_out):
        tok = jnp.stack([x_blk.reshape(T, D), y_blk.reshape(T, D)])
        own = lax.ppermute(tok, axes, move_pairs(sub_size, data_size, 0))
        other = lax.ppermute(tok, axes, move_pairs(sub_size, data_size, 1))
        v_in, v_out = w_in.astype(BF16), w_out.astype(BF16)
        first = tuple(run_pass(own[0], own[1], v_in, v_out)[:2])
        second = run_pass(other[0], other[1], v_in, v_out, first)
        t_in, t_out = ascent(sub_size, first, second[:2], second[3:], w_in, w_out)
        new_in, new_out, loss_all = last_pass(dev_count, own[0], own[1], t_in, t_out, w_in, w_out)
        return new_in, new_out, loss_all[0, 0]

    batch_spec = P(("data", "sub"))
    return jax.shard_map(device_step, mesh=mesh, in_specs=(batch_spec, batch_spec, P(), P()), out_specs=(P(), P(), P()), check_vma=False)
```

```python
import jax, jax.numpy as jnp, functools
from jax import lax
from jax.experimental import pallas as pl
from jax.experimental.pallas import tpu as pltpu
from jax.sharding import PartitionSpec as P

F32, BF16 = jnp.float32, jnp.bfloat16
RHO_SCALE = 0.1
STEP_SIZE = 1.0
L, T, D, F = 8, 784, 384, 1536
FT = 256
NT = F // FT
RC, CC = 16, 256
SQRT_HALF = 0.5 ** 0.5
INV_SQRT_2PI = 0.3989422804014327


def gelu_only(z):
    return z * (0.5 + 0.5 * lax.erf(z * SQRT_HALF))


def gelu_both(z):
    cdf = 0.5 + 0.5 * lax.erf(z * SQRT_HALF)
    pdf = INV_SQRT_2PI * jnp.exp(-0.5 * (z * z))
    return z * cdf, cdf + z * pdf


def chunks(col0):
    for c in range(FT // CC):
        for r in range(T // RC):
            yield slice(r * RC, (r + 1) * RC), slice(col0 + c * CC, col0 + (c + 1) * CC)


def dot(a, b, ca=1, cb=0):
    return lax.dot_general(a, b, (((ca,), (cb,)), ((), ())), preferred_element_type=F32)


def pass_kernel(x_ref, y_ref, vin_ref, vout_ref, gin_ref, gout_ref, loss_ref, h_s, z_s, a_s, q_s, e_s, hT_s):
    step = pl.program_id(0)

    @pl.when(step == 0)
    def _():
        h_s[0] = x_ref[...]

    @pl.when(step < L)
    def _():
        lay = step
        z_l = z_s.at[lay]
        h = h_s[lay]
        def pre(j):
            cols = slice(j * FT, (j + 1) * FT)
            z_l[:, cols] = dot(h, vin_ref[0, :, cols]).astype(BF16)

        pre(0)
        for j in range(NT):
            if j + 1 < NT:
                pre(j + 1)
            for rs, cs in chunks(j * FT):
                a_s[rs, cs] = gelu_only(z_l[rs, cs].astype(F32)).astype(BF16)
        out = (h.astype(F32) + dot(a_s[...], vout_ref[0])).astype(BF16)
        h_s[lay + 1] = out

    @pl.when(step == L - 1)
    def _():
        diff = h_s[L].astype(F32) - y_ref[...].astype(F32)
        loss_ref[0, 0] = 0.5 * jnp.sum(diff * diff) / (T * D)
        e_s[...] = (diff / (T * D)).astype(BF16)

    @pl.when(step >= L)
    def _():
        lay = 2 * L - 1 - step
        z_l = z_s.at[lay]
        e = e_s[...]
        hT_s[...] = h_s[lay].T
        def up(j):
            cols = slice(j * FT, (j + 1) * FT)
            q_s[:, cols] = dot(e, vout_ref[0, cols, :], 1, 1).astype(BF16)

        up(0)
        for j in range(NT):
            if j + 1 < NT:
                up(j + 1)
            for rs, cs in chunks(j * FT):
                act, slope = gelu_both(z_l[rs, cs].astype(F32))
                a_s[rs, cs] = act.astype(BF16)
                q_s[rs, cs] = (slope * q_s[rs, cs].astype(F32)).astype(BF16)
        gout_ref[0] = dot(a_s[...], e, 0, 0).astype(BF16)
        gin_ref[0] = dot(hT_s[...], q_s[...]).astype(BF16)
        e_s[...] = (e.astype(F32) + dot(q_s[...], vin_ref[0], 1, 1)).astype(BF16)


def swap_pass_kernel(x_ref, y_ref, vin_ref, vout_ref, a0, a1, gin_ref, gout_ref, loss_ref, p0, p1, h_s, z_s, a_s, q_s, e_s, hT_s, s_sem, r_sem):
    me = Place()
    src, dst = (a0, a1), (p0, p1)

    def copy(l, k):
        return remote(half_at(src[k], k, l, 1 - me.core, 0, ROWS[k]), dst[k].at[l], s_sem.at[l, k], r_sem.at[l, k], me.partner)

    step = pl.program_id(0)

    @pl.when(step == 0)
    def _():
        me.barrier([me.partner])

    @pl.when(step < L)
    def _():
        for k in (0, 1):
            copy(step, k).start()
    pass_kernel(x_ref, y_ref, vin_ref, vout_ref, gin_ref, gout_ref, loss_ref, h_s, z_s, a_s, q_s, e_s, hT_s)

    @pl.when(step == 2 * L - 1)
    def _():
        def end(l, _):
            for k in (0, 1):
                copy(l, k).wait()
            return 0
        lax.fori_loop(0, L, end, 0)


def run_pass(x, y, vin, vout, earlier=()):
    lay = lambda s: jnp.where(s < L, s, 2 * L - 1 - s)
    glay = lambda s: jnp.where(s < L, L - 1, 2 * L - 1 - s)
    any_spec = pl.BlockSpec(memory_space=pl.ANY)
    extra = [any_spec] * len(earlier)
    landed = [jax.ShapeDtypeStruct((L, ROWS[k], COLS[k]), BF16) for k in range(len(earlier))]
    sems = [pltpu.SemaphoreType.DMA((L, 2))] * len(earlier)
    more = dict(collective_id=3, has_side_effects=True) if earlier else {}
    return pl.pallas_call(
        swap_pass_kernel if earlier else pass_kernel,
        grid=(2 * L,),
        in_specs=[
            pl.BlockSpec((T, D), lambda s: (0, 0)),
            pl.BlockSpec((T, D), lambda s: (0, 0)),
            pl.BlockSpec((1, D, F), lambda s: (lay(s), 0, 0)),
            pl.BlockSpec((1, F, D), lambda s: (lay(s), 0, 0)),
        ] + extra,
        out_specs=[
            pl.BlockSpec((1, D, F), lambda s: (glay(s), 0, 0)),
            pl.BlockSpec((1, F, D), lambda s: (glay(s), 0, 0)),
            pl.BlockSpec(memory_space=pltpu.SMEM),
        ] + extra,
        out_shape=[
            jax.ShapeDtypeStruct((L, D, F), BF16),
            jax.ShapeDtypeStruct((L, F, D), BF16),
            jax.ShapeDtypeStruct((1, 1), F32),
        ] + landed,
        scratch_shapes=[
            pltpu.VMEM((L + 1, T, D), BF16),
            pltpu.VMEM((L, T, F), BF16),
            pltpu.VMEM((T, F), BF16),
            pltpu.VMEM((T, F), BF16),
            pltpu.VMEM((T, D), BF16),
            pltpu.VMEM((D, T), BF16),
        ] + sems,
        compiler_params=pltpu.CompilerParams(vmem_limit_bytes=60 * 2**20, **more),
        cost_estimate=pl.CostEstimate(flops=L * 12 * T * D * F, bytes_accessed=4 * L * D * F * 2, transcendentals=0),
    )(x, y, vin, vout, *earlier)


ROWS = (384, 768)
COLS = (768, 384)
STAGES = 7
MESH_ID = pl.DeviceIdType.MESH


def al(v, n):
    return pl.multiple_of(v, n)


def half_at(ref, kind, lay, core, row, rows):
    if kind == 0:
        return ref.at[lay, pl.ds(al(row, 8), rows), pl.ds(al(core * COLS[0], 128), COLS[0])]
    return ref.at[lay, pl.ds(al(core * ROWS[1] + row, 8), rows), :]


def row_loop(rows, block, body):
    def step(i, _):
        body(al(i * block, block))
        return 0
    lax.fori_loop(0, rows // block, step, 0)


class Place:
    def __init__(self):
        z, data = lax.axis_index("sub"), lax.axis_index("data")
        core, xx, yy = lax.rem(data, 2), lax.rem(data // 2, 2), data // 4
        self.core, self.z = core, z
        flips = (2 - 4 * xx, 4 - 8 * yy)
        self.partner = (z, data + 1 - 2 * core)
        self.first = tuple((z, data + f) for f in flips)
        self.second = (self.first[1], self.first[0])
        self.c1, self.c2 = (xx, yy), (yy, xx)
        self.zs = [lax.rem(z + d, 4) for d in (1, 2, 3)]
        self.z_peers = [(zt, data) for zt in self.zs]

    def barrier(self, peers):
        sem = pltpu.get_barrier_semaphore()
        for peer in peers:
            pl.semaphore_signal(sem, inc=1, device_id=peer, device_id_type=MESH_ID)
        pl.semaphore_wait(sem, len(peers))


def remote(src, dst, send, recv, peer):
    return pltpu.make_async_remote_copy(src_ref=src, dst_ref=dst, send_sem=send, recv_sem=recv, device_id=peer, device_id_type=MESH_ID)


def last_kernel(count, x_ref, y_ref, vin_ref, vout_ref, w0, w1, o0, o1, lout, h_s, z_s, a_s, q_s, e_s, hT_s, gs0, gs1,
                d0, d1, r10, r11, r20, r21, r30, r31, s10, s11, s20, s21, s30, s31, nb0, nb1, wb0, wb1, lt, lr,
                w_sem, d_sem, r1_sem, r2_sem, r3_sem, az_sem, a2_sem, a1_sem, ad_sem,
                ds_sem, s1_sem, s2_sem, s3_sem, zs_sem, n_sem, a2s_sem, a1s_sem, ads_sem, l_sem, ls_sem):
    step = pl.program_id(0)
    me = Place()
    core, z = me.core, me.z
    gs, w, o = (gs0, gs1), (w0, w1), (o0, o1)
    dd, r1, r2, r3 = (d0, d1), (r10, r11), (r20, r21), (r30, r31)
    s1, s2, s3, nb, wb = (s10, s11), (s20, s21), (s30, s31), (nb0, nb1), (wb0, wb1)
    kinds = (0, 1)

    def quarter(kind):
        return (2 * me.c1[kind] + me.c2[kind]) * (ROWS[kind] // 4)

    def w_copy(l, k):
        n = ROWS[k] // 16
        return pltpu.make_async_copy(half_at(w[k], k, L - 1 - l, core, quarter(k) + z * n, n), wb[k].at[l], w_sem.at[l, k])

    def d_copy(l, k):
        slot = lax.rem(l, 3)
        return remote(half_at(gs[k], k, slot, 1 - core, 0, ROWS[k]), dd[k].at[l], ds_sem.at[slot, k], d_sem.at[l, k], me.partner)

    def r1_copy(l, k):
        slot = lax.rem(l, 2)
        return remote(s1[k].at[slot], r1[k].at[l], s1_sem.at[slot, k], r1_sem.at[l, k], me.first[k])

    def r2_copy(l, k):
        slot = lax.rem(l, 2)
        return remote(s2[k].at[slot], r2[k].at[l], s2_sem.at[slot, k], r2_sem.at[l, k], me.second[k])

    def r3_copy(l, k, j):
        slot, n = lax.rem(l, 2), ROWS[k] // 16
        return remote(s3[k].at[slot, pl.ds(al(me.zs[j] * n, 8), n)], r3[k].at[l, 2 - j], s3_sem.at[slot, k, j], r3_sem.at[l, k, 2 - j], me.z_peers[j])

    def piece(l, k, zi):
        n = ROWS[k] // 16
        return half_at(o[k], k, L - 1 - l, core, quarter(k) + zi * n, n)

    def az_copy(l, k, j):
        slot = lax.rem(l, 2)
        return remote(nb[k].at[slot], piece(l, k, z), zs_sem.at[slot, k, j], az_sem.at[l, k, 2 - j], me.z_peers[j])

    def n_copy(l, k):
        slot = lax.rem(l, 2)
        return pltpu.make_async_copy(nb[k].at[slot], piece(l, k, z), n_sem.at[slot, k])

    def gather(l, k, row, rows, send, recv, peer):
        part = half_at(o[k], k, L - 1 - l, core, row, rows)
        return remote(part, part, send.at[lax.rem(l, 2), k], recv.at[l, k], peer)

    def a2_copy(l, k):
        return gather(l, k, quarter(k), ROWS[k] // 4, a2s_sem, a2_sem, me.second[k])

    def a1_copy(l, k):
        return gather(l, k, me.c1[k] * (ROWS[k] // 2), ROWS[k] // 2, a1s_sem, a1_sem, me.first[k])

    def ad_copy(l, k):
        return gather(l, k, 0, ROWS[k], ads_sem, ad_sem, me.partner)

    def both(k, l, row, n):
        slot = lax.rem(l, 3)
        if k == 0:
            mine = gs[0][slot, pl.ds(row, n), pl.ds(al(core * COLS[0], 128), COLS[0])]
        else:
            mine = gs[1][slot, pl.ds(al(core * ROWS[1] + row, 16), n), :]
        return mine.astype(F32) + dd[k][l, pl.ds(row, n), :].astype(F32)

    def stage0(l, k):
        d_copy(l, k).wait_recv()

        @pl.when(l >= 2)
        def _():
            r1_copy(l - 2, k).wait_send()
        n, slot = ROWS[k] // 2, lax.rem(l, 2)
        base = (1 - me.c1[k]) * n

        def body(row):
            s1[k][slot, pl.ds(row, 16), :] = both(k, l, al(base + row, 16), 16)
        row_loop(n, 16, body)
        r1_copy(l, k).start()

    def stage1(l, k):
        r1_copy(l, k).wait_recv()

        @pl.when(l >= 2)
        def _():
            r2_copy(l - 2, k).wait_send()
        n, slot = ROWS[k] // 4, lax.rem(l, 2)
        in_half = (1 - me.c2[k]) * n
        base = me.c1[k] * 2 * n + in_half

        def body(row):
            s2[k][slot, pl.ds(row, 16), :] = both(k, l, al(base + row, 16), 16) + r1[k][l, pl.ds(al(in_half + row, 16), 16), :]
        row_loop(n, 16, body)
        r2_copy(l, k).start()

    def stage2(l, k):
        r2_copy(l, k).wait_recv()

        @pl.when(l >= 2)
        def _():
            for j in range(3):
                r3_copy(l - 2, k, j).wait_send()
        n, slot = ROWS[k] // 4, lax.rem(l, 2)
        in_half = me.c2[k] * n
        base = me.c1[k] * 2 * n + in_half

        def body(row):
            s3[k][slot, pl.ds(row, 16), :] = (both(k, l, al(base + row, 16), 16) + r1[k][l, pl.ds(al(in_half + row, 16), 16), :]) + r2[k][l, pl.ds(row, 16), :]
        row_loop(n, 16, body)
        for j in range(3):
            r3_copy(l, k, j).start()

    def stage3(l, k):
        for j in range(3):
            r3_copy(l, k, j).wait_recv()
        w_copy(l, k).wait()

        @pl.when(l >= 2)
        def _():
            for j in range(3):
                az_copy(l - 2, k, j).wait_send()
        n, slot = ROWS[k] // 16, lax.rem(l, 2)

        def body(row):
            rs = pl.ds(row, 8)
            tot = (s3[k][slot, pl.ds(al(z * n + row, 8), 8), :] + r3[k][l, 0, rs, :]) + (r3[k][l, 1, rs, :] + r3[k][l, 2, rs, :])
            nb[k][slot, rs, :] = wb[k][l, rs, :] - STEP_SIZE * (tot * (1.0 / count))
        row_loop(n, 8, body)
        n_copy(l, k).start()
        for j in range(3):
            az_copy(l, k, j).start()

    def stage4(l, k):
        n_copy(l, k).wait()
        for j in range(3):
            az_copy(l, k, j).wait_recv()

        @pl.when(l >= 2)
        def _():
            a2_copy(l - 2, k).wait_send()
        a2_copy(l, k).start()

    def stage5(l, k):
        a2_copy(l, k).wait_recv()

        @pl.when(l >= 2)
        def _():
            a1_copy(l - 2, k).wait_send()
        a1_copy(l, k).start()

    def stage6(l, k):
        a1_copy(l, k).wait_recv()

        @pl.when(l >= 2)
        def _():
            ad_copy(l - 2, k).wait_send()
        ad_copy(l, k).start()

    stages = (stage0, stage1, stage2, stage3, stage4, stage5, stage6)

    def loss_copy(i, peer, j):
        return remote(lt.at[i], lr.at[j], ls_sem.at[j], l_sem.at[j], peer)

    loss_hops = [[(me.partner, 0)], [(me.first[0], 1)], [(me.first[1], 2)], [(me.z_peers[j], 3 + j) for j in range(3)]]

    def loss_wait(i):
        for peer, j in loss_hops[i]:
            loss_copy(i, peer, j).wait()
        tot = lt[i]
        for _, j in loss_hops[i]:
            tot = tot + (lr[j] if i < 3 else lr[8 - j])
        return tot

    def start_all(l, _):
        for k in kinds:
            w_copy(l, k).start()
        return 0

    def loss_step(t):
        for i in range(5):
            @pl.when(t == i)
            def _(i=i):
                if i > 0:
                    tot = loss_wait(i - 1)
                    if i == 4:
                        lout[...] = tot * (1.0 / count)
                    else:
                        lt[i] = tot
                if i < 4:
                    for peer, j in loss_hops[i]:
                        loss_copy(i, peer, j).start()

    def tick(t, _):
        loss_step(t)

        @pl.when(t < L)
        def _():
            for k in kinds:
                d_copy(t, k).start()
        for s in reversed(range(STAGES)):
            l = t - s

            @pl.when(jnp.logical_and(l >= 0, l < L))
            def _(s=s, l=l):
                for k in kinds:
                    stages[s](l, k)
        return 0

    @pl.when(step == 0)
    def _():
        me.barrier([me.partner, me.first[0], me.first[1]] + me.z_peers)
        h_s[0] = x_ref[...]
        lax.fori_loop(0, L, start_all, 0)

    @pl.when(step < L)
    def _():
        h = h_s[step]
        for j in range(NT):
            cols = slice(j * FT, (j + 1) * FT)
            z_s[:, cols] = dot(h, vin_ref[0, :, cols]).astype(BF16)
            for rs, cs in chunks(j * FT):
                a_s[rs, cs] = gelu_only(z_s[rs, cs].astype(F32)).astype(BF16)
        h_s[step + 1] = (h.astype(F32) + dot(a_s[...], vout_ref[0])).astype(BF16)

    @pl.when(step == L - 1)
    def _():
        diff = h_s[L].astype(F32) - y_ref[...].astype(F32)
        lt[0] = jnp.full((8, 128), 0.5 * jnp.sum(diff * diff) / (T * D), F32)
        e_s[...] = (diff / (T * D)).astype(BF16)

    @pl.when(step >= L)
    def _():
        item = step - L
        slot = lax.rem(item, 3)
        lay = L - 1 - item

        @pl.when(item >= 3)
        def _():
            for k in kinds:
                d_copy(item - 3, k).wait_send()
        e, h = e_s[...], h_s[lay]
        hT_s[...] = h.T
        for j in range(NT):
            cols = slice(j * FT, (j + 1) * FT)
            z_s[:, cols] = dot(h, vin_ref[0, :, cols]).astype(BF16)
            q_s[:, cols] = dot(e, vout_ref[0, cols, :], 1, 1).astype(BF16)
            for rs, cs in chunks(j * FT):
                act, slope = gelu_both(z_s[rs, cs].astype(F32))
                a_s[rs, cs] = act.astype(BF16)
                q_s[rs, cs] = (slope * q_s[rs, cs].astype(F32)).astype(BF16)
            gs1[slot, cols, :] = dot(a_s[:, cols], e, 0, 0).astype(BF16)
            gs0[slot, :, cols] = dot(hT_s[...], q_s[:, cols]).astype(BF16)
        e_s[...] = (e.astype(F32) + dot(q_s[...], vin_ref[0], 1, 1)).astype(BF16)
        lax.fori_loop(item, jnp.where(item == L - 1, L + STAGES - 1, item + 1), tick, 0)

    @pl.when(step == 2 * L - 1)
    def _():
        def finish(l, _):
            for k in kinds:
                ad_copy(l, k).wait_recv()
            return 0
        lax.fori_loop(0, L, finish, 0)
        for l in (L - 3, L - 2, L - 1):
            for k in kinds:
                d_copy(l, k).wait_send()
        for l in (L - 2, L - 1):
            for k in kinds:
                r1_copy(l, k).wait_send()
                r2_copy(l, k).wait_send()
                for j in range(3):
                    r3_copy(l, k, j).wait_send()
                    az_copy(l, k, j).wait_send()
                a2_copy(l, k).wait_send()
                a1_copy(l, k).wait_send()
                ad_copy(l, k).wait_send()


def last_pass(count, x, y, vin, vout, w_in, w_out):
    def per_kind(lead, div, dtype):
        return [pltpu.VMEM(lead + (ROWS[k] // div, COLS[k]), dtype) for k in (0, 1)]
    dma = pltpu.SemaphoreType.DMA
    any_spec = pl.BlockSpec(memory_space=pl.ANY)
    lay = lambda s: jnp.where(s < L, s, 2 * L - 1 - s)
    scratch = ([pltpu.VMEM((L + 1, T, D), BF16)] + [pltpu.VMEM((T, F), BF16)] * 3 + [pltpu.VMEM((T, D), BF16), pltpu.VMEM((D, T), BF16)]
               + [pltpu.VMEM((3, D, F), BF16), pltpu.VMEM((3, F, D), BF16)]
               + per_kind((L,), 1, BF16) + per_kind((L,), 2, F32) + per_kind((L,), 4, F32)
               + per_kind((L, 3), 16, F32) + per_kind((2,), 2, F32) + per_kind((2,), 4, F32) + per_kind((2,), 4, F32)
               + per_kind((2,), 16, F32) + per_kind((L,), 16, F32) + [pltpu.VMEM((4, 8, 128), F32), pltpu.VMEM((6, 8, 128), F32)]
               + [dma((L, 2))] * 4 + [dma((L, 2, 3))] * 2 + [dma((L, 2))] * 3 + [dma((3, 2))]
               + [dma((2, 2))] * 2 + [dma((2, 2, 3))] * 2 + [dma((2, 2))] * 4 + [dma((6,))] * 2)
    return pl.pallas_call(
        functools.partial(last_kernel, count),
        grid=(2 * L,),
        in_specs=[
            pl.BlockSpec((T, D), lambda s: (0, 0), pipeline_mode=pl.Buffered(1)),
            pl.BlockSpec((T, D), lambda s: (0, 0), pipeline_mode=pl.Buffered(1)),
            pl.BlockSpec((1, D, F), lambda s: (lay(s), 0, 0)),
            pl.BlockSpec((1, F, D), lambda s: (lay(s), 0, 0)),
            any_spec,
            any_spec,
        ],
        out_specs=[any_spec, any_spec, pl.BlockSpec((8, 128), lambda s: (0, 0))],
        out_shape=[jax.ShapeDtypeStruct((L, D, F), F32), jax.ShapeDtypeStruct((L, F, D), F32), jax.ShapeDtypeStruct((8, 128), F32)],
        scratch_shapes=scratch,
        compiler_params=pltpu.CompilerParams(collective_id=1, has_side_effects=True, vmem_limit_bytes=67_000_000),
    )(x, y, vin, vout, w_in, w_out)


def ascent_kernel(group, a0, a1, b0, b1, h0, h1, w0, w1, t0, t1, oa0, oa1, ob0, ob1, pa0, pa1, pb0, pb1, wb0, wb1, tb0, tb1, nt,
                  o_sem, p_sem, ps_sem, w_sem, tl_sem, ts_sem, tr_sem, n_sem):
    me = Place()
    core = me.core
    src, w, t = ((a0, a1), (b0, b1)), (w0, w1), (t0, t1)
    own, peer = ((oa0, oa1), (ob0, ob1)), ((pa0, pa1), (pb0, pb1))
    wb, tb, kinds = (wb0, wb1), (tb0, tb1), (0, 1)
    me.barrier([me.partner])

    def own_copy(l, k, i):
        return pltpu.make_async_copy(half_at(src[i][k], k, l, core, 0, ROWS[k]), own[i][k].at[l], o_sem.at[l, k, i])

    def peer_copy(l, k, i):
        if i == 0:
            return pltpu.make_async_copy((h0, h1)[k].at[l], peer[0][k].at[l], p_sem.at[l, k, 0])
        return remote(half_at(src[i][k], k, l, 1 - core, 0, ROWS[k]), peer[i][k].at[l], ps_sem.at[l, k, i], p_sem.at[l, k, i], me.partner)

    def w_copy(l, k):
        slot = lax.rem(l, 2)
        return pltpu.make_async_copy(half_at(w[k], k, l, core, 0, ROWS[k]), wb[k].at[slot], w_sem.at[slot, k])

    def t_half(l, k):
        return half_at(t[k], k, l, core, 0, ROWS[k])

    def t_local(l, k):
        slot = lax.rem(l, 2)
        return pltpu.make_async_copy(tb[k].at[slot], t_half(l, k), tl_sem.at[slot, k])

    def t_send(l, k):
        slot = lax.rem(l, 2)
        return remote(tb[k].at[slot], t_half(l, k), ts_sem.at[slot, k], tr_sem.at[l, k], me.partner)

    def mean_rows(l, k, row):
        rs = pl.ds(row, 16)
        f = lambda ref: ref[l, rs, :].astype(F32)
        return ((f(own[0][k]) + f(own[1][k])) + (f(peer[0][k]) + f(peer[1][k]))) * (1.0 / group)

    def start_all(l, _):
        for k in kinds:
            for i in (1, 0):
                peer_copy(l, k, i).start()
                own_copy(l, k, i).start()
        return 0
    lax.fori_loop(0, L, start_all, 0)
    for l in range(2):
        for k in kinds:
            w_copy(l, k).start()

    def square_layer(l, acc):
        for k in kinds:
            own_copy(l, k, 0).wait()
            own_copy(l, k, 1).wait()
            peer_copy(l, k, 0).wait()
            peer_copy(l, k, 1).wait_recv()

            def body(i, tot, k=k):
                g = mean_rows(l, k, al(i * 16, 16))
                sq = g * g
                parts = [sq[r:r + 8, c:c + 128] for r in (0, 8) for c in range(0, COLS[k], 128)]
                while len(parts) > 1:
                    parts = [u + v for u, v in zip(parts[::2], parts[1::2])] + parts[len(parts) & ~1:]
                return tot + parts[0]
            acc = lax.fori_loop(0, ROWS[k] // 16, body, acc)
        return acc
    nt[0] = lax.fori_loop(0, L, square_layer, jnp.zeros((8, 128), F32))
    norm_copy = remote(nt.at[0], nt.at[1], n_sem.at[0], n_sem.at[1], me.partner)
    norm_copy.start()
    norm_copy.wait()
    total = jnp.sum(jnp.sum(nt[0] + nt[1], axis=0, keepdims=True), axis=1, keepdims=True)
    scale = (RHO_SCALE * D ** 0.5) / jnp.sqrt(total)

    def move_layer(l, _):
        for k in kinds:
            slot = lax.rem(l, 2)
            w_copy(l, k).wait()

            @pl.when(l >= 2)
            def _(k=k):
                t_local(l - 2, k).wait()
                t_send(l - 2, k).wait_send()

            def body(row, k=k, slot=slot):
                rs = pl.ds(row, 16)
                tb[k][slot, rs, :] = (wb[k][slot, rs, :] + scale * mean_rows(l, k, row)).astype(BF16)
            row_loop(ROWS[k], 16, body)
            t_send(l, k).start()
            t_local(l, k).start()

            @pl.when(l < L - 2)
            def _(k=k):
                w_copy(l + 2, k).start()
        return 0
    lax.fori_loop(0, L, move_layer, 0)

    def finish(l, _):
        for k in kinds:
            t_send(l, k).wait_recv()
            peer_copy(l, k, 1).wait_send()
        return 0
    lax.fori_loop(0, L, finish, 0)
    for l in (L - 2, L - 1):
        for k in kinds:
            t_local(l, k).wait()
            t_send(l, k).wait_send()


def ascent(group, first, second, landed, w_in, w_out):
    def per_kind(lead, dtype):
        return [pltpu.VMEM((lead, ROWS[k], COLS[k]), dtype) for k in (0, 1)]
    dma = pltpu.SemaphoreType.DMA
    any_spec = pl.BlockSpec(memory_space=pl.ANY)
    scratch = (per_kind(L, BF16) * 4 + per_kind(2, F32) + per_kind(2, BF16) + [pltpu.VMEM((2, 8, 128), F32)]
               + [dma((L, 2, 2))] * 3 + [dma((2, 2))] * 3 + [dma((L, 2)), dma((2,))])
    return pl.pallas_call(
        functools.partial(ascent_kernel, group),
        in_specs=[any_spec] * 8,
        out_specs=[any_spec] * 2,
        out_shape=[jax.ShapeDtypeStruct((L, D, F), BF16), jax.ShapeDtypeStruct((L, F, D), BF16)],
        scratch_shapes=scratch,
        compiler_params=pltpu.CompilerParams(collective_id=2, has_side_effects=True, vmem_limit_bytes=60 * 2**20),
    )(*first, *second, *landed, w_in, w_out)


def move_pairs(sub_size, data_size, flip):
    pairs = []
    for shard in range(sub_size):
        for data_idx in range(data_size):
            group = data_idx % 2
            chip = 2 * ((shard // 2 + flip) % 2) + group
            pairs.append((shard * data_size + data_idx, chip * data_size + data_idx - group + shard % 2))
    return pairs


def solution(mesh):
    sub_size, data_size = mesh.shape["sub"], mesh.shape["data"]
    dev_count = sub_size * data_size
    axes = ("sub", "data")

    def device_step(x_blk, y_blk, w_in, w_out):
        tok = jnp.stack([x_blk.reshape(T, D), y_blk.reshape(T, D)])
        own = lax.ppermute(tok, axes, move_pairs(sub_size, data_size, 0))
        other = lax.ppermute(tok, axes, move_pairs(sub_size, data_size, 1))
        v_in, v_out = w_in.astype(BF16), w_out.astype(BF16)
        first = tuple(run_pass(own[0], own[1], v_in, v_out)[:2])
        second = run_pass(other[0], other[1], v_in, v_out, first)
        t_in, t_out = ascent(sub_size, first, second[:2], second[3:], w_in, w_out)
        new_in, new_out, loss_all = last_pass(dev_count, own[0], own[1], t_in, t_out, w_in, w_out)
        return new_in, new_out, loss_all[0, 0]

    batch_spec = P(("data", "sub"))
    return jax.shard_map(device_step, mesh=mesh, in_specs=(batch_spec, batch_spec, P(), P()), out_specs=(P(), P(), P()), check_vma=False)
```
